32 devices in a mesh: batch: 1 (over z), col: 4 (over y), row: 8 (over x, core).
Axes of the slice: x: 4, y: 4, z: 1, core: 2. Of those that a mesh axis runs over, the one named last changes fastest.
The devices are a block of a 4x4x8 slice.
Arguments:
- images: bfloat16 [16, 256, 512, 64], P('batch', 'row', 'col')
- w_down1: bfloat16 [4, 4, 64, 128], replicated
- b_down1: float32 [128], replicated
- w_conv1: bfloat16 [3, 3, 128, 128], replicated
- b_conv1: float32 [128], replicated
- w_down2: bfloat16 [4, 4, 128, 256], replicated
- b_down2: float32 [256], replicated
- w_conv2: bfloat16 [3, 3, 256, 256], replicated
- b_conv2: float32 [256], replicated
- w_down3: bfloat16 [4, 4, 256, 320], replicated
- b_down3: float32 [320], replicated
- w_conv3: bfloat16 [3, 3, 320, 320], replicated
- b_conv3: float32 [320], replicated
Outputs:
- output: bfloat16 [16, 32, 64, 320], P('batch', 'row', 'col')
All inputs are finite; a program needn't handle non-finite values.
Results may differ from the reference program's by a relative error of at most 0.00703317.
Values are sent between devices in bfloat16 or wider.
A program may use at most 768 MiB of HBM per device.

```python
import jax
import jax.numpy as jnp
from jax import lax

NUM_IMAGES = 16
IMG_HEIGHT = 256
IMG_WIDTH = 512
CH_IN = 64
CH_ONE = 128
CH_TWO = 256
CH_THREE = 320


def setup_inputs(seed: int = 0, part: int = 0) -> dict:
    key_list = jax.random.split(jax.random.key(seed), 13)
    image_key = jax.random.fold_in(key_list[0], part)
    images = jax.random.normal(image_key, (NUM_IMAGES, IMG_HEIGHT, IMG_WIDTH, CH_IN), jnp.float32)
    drawn_args = {'images': images.astype(jnp.bfloat16)}
    widths = [CH_IN, CH_ONE, CH_TWO, CH_THREE]
    for stage_idx in range(3):
        c_in = widths[stage_idx]
        c_out = widths[stage_idx + 1]
        key_base = 1 + 4 * stage_idx
        w_down = jax.random.normal(key_list[key_base], (4, 4, c_in, c_out), jnp.float32) * (2.0 / (16 * c_in)) ** 0.5
        b_down = 0.25 * jax.random.normal(key_list[key_base + 1], (c_out,), jnp.float32)
        w_conv = jax.random.normal(key_list[key_base + 2], (3, 3, c_out, c_out), jnp.float32) * (2.0 / (9 * c_out)) ** 0.5
        b_conv = 0.25 * jax.random.normal(key_list[key_base + 3], (c_out,), jnp.float32)
        suffix = str(stage_idx + 1)
        drawn_args['w_down' + suffix] = w_down.astype(jnp.bfloat16)
        drawn_args['b_down' + suffix] = b_down
        drawn_args['w_conv' + suffix] = w_conv.astype(jnp.bfloat16)
        drawn_args['b_conv' + suffix] = b_conv
    return drawn_args


def conv_relu(act_in, weight, bias_vec, stride):
    summed = lax.conv_general_dilated(act_in.astype(jnp.float32), weight.astype(jnp.float32), (stride, stride), ((1, 1), (1, 1)), dimension_numbers=('NHWC', 'HWIO', 'NHWC'))
    return jax.nn.relu(summed + bias_vec).astype(jnp.bfloat16)


def reference(images, w_down1, b_down1, w_conv1, b_conv1, w_down2, b_down2, w_conv2, b_conv2, w_down3, b_down3, w_conv3, b_conv3):
    params = [(w_down1, b_down1, w_conv1, b_conv1), (w_down2, b_down2, w_conv2, b_conv2), (w_down3, b_down3, w_conv3, b_conv3)]

    def encode(one_image):
        act_tile = one_image[None]
        for w_down, b_down, w_conv, b_conv in params:
            act_tile = conv_relu(act_tile, w_down, b_down, 2)
            act_tile = conv_relu(act_tile, w_conv, b_conv, 1)
        return act_tile[0]

    return lax.map(encode, images)
```

```python
import functools

import jax
import jax.numpy as jnp
from jax import lax
from jax.experimental import pallas as pl
from jax.experimental.pallas import tpu as pltpu
from jax.sharding import PartitionSpec as P

BY_LAST = (((1,), (1,)), ((), ()))
BF = jnp.bfloat16
F32 = jnp.float32
LANES = 128
TILE = 2 * LANES
PITCH = 136


def _encoder_kernel(dims, img, wd1, bd1, wc1, bc1, wd2, bd2, wc2, bc2, wd3, bd3, wc3, bc3, out,
                    raw, xt, y1, z1, y2, z2, y3, st0, st1, st2,
                    vwd1, vwc1, vwd2, vwc2, vwd3, vwc3, wp1, wp2, wp6,
                    vb1, vb2, vb3, vb4, vb5, vb6,
                    raw_sem, w_sem, rh_send, rh_recv, xc_send, xc_recv,
                    row_send, row_recv, cor_send, cor_recv, col_send, col_recv):
    row_len, col_len = dims
    nimg = img.shape[0]
    my_row = lax.axis_index('row')
    my_col = lax.axis_index('col')
    up, down = my_row > 0, my_row < row_len - 1
    left, right = my_col > 0, my_col < col_len - 1

    def both(a, b):
        return jnp.logical_and(a, b)

    near = [(up, -1, 0), (down, 1, 0), (left, 0, -1), (right, 0, 1)]
    near += [(both(v[0], g[0]), v[1], g[2]) for v in near[:2] for g in near[2:]]

    def dev(dr, dc):
        return {'row': my_row + dr, 'col': my_col + dc}

    def raw_copy(k):
        return pltpu.make_async_copy(img.at[:, pl.ds(2 * k - 1, 2)], raw.at[k], raw_sem.at[k])

    last = raw.shape[0] - 1
    mid = last // 2
    first_copy = pltpu.make_async_copy(img.at[:, pl.ds(0, 1)], raw.at[0, :, pl.ds(1, 1)], raw_sem.at[0])
    last_copy = pltpu.make_async_copy(img.at[:, pl.ds(2 * last - 1, 1)], raw.at[last, :, pl.ds(0, 1)], raw_sem.at[last])
    order = []
    for t in range(last - 1):
        h = (t + 1) // 2
        order.append(mid - h if t % 2 else mid + h)
    for k in order[:3]:
        raw_copy(k).start()
    weights = [(wd1, vwd1), (wc1, vwc1), (wd2, vwd2), (wc2, vwc2), (wd3, vwd3), (wc3, vwc3),
               (bd1, vb1), (bc1, vb2), (bd2, vb3), (bc2, vb4), (bd3, vb5), (bc3, vb6)]
    wcopies = [pltpu.make_async_copy(s, d, w_sem.at[i]) for i, (s, d) in enumerate(weights)]
    for i in (0, 6, 1, 7):
        wcopies[i].start()
    for k in order[3:]:
        raw_copy(k).start()
    first_copy.start()
    last_copy.start()
    for i in (2, 8, 3, 9, 4, 10, 5, 11):
        wcopies[i].start()

    barrier = pltpu.get_barrier_semaphore()
    for there, dr, dc in near:
        @pl.when(there)
        def _(dr=dr, dc=dc):
            pl.semaphore_signal(barrier, inc=1, device_id=dev(dr, dc), device_id_type=pl.DeviceIdType.MESH)
    nu, nd, nl, nr = [jnp.where(x, 1, 0) for x in (up, down, left, right)]
    pl.semaphore_wait(barrier, (1 + nu + nd) * (1 + nl + nr) - 1)

    def raw_send(s):
        if s == 0:
            return pltpu.make_async_remote_copy(img.at[:, pl.ds(0, 1)], raw.at[last, :, pl.ds(1, 1)],
                                                rh_send.at[0], rh_recv.at[0], device_id=dev(-1, 0), device_id_type=pl.DeviceIdType.MESH)
        return pltpu.make_async_remote_copy(img.at[:, pl.ds(2 * last - 1, 1)], raw.at[0, :, pl.ds(0, 1)],
                                            rh_send.at[1], rh_recv.at[1], device_id=dev(1, 0), device_id_type=pl.DeviceIdType.MESH)

    for there, s in zip((up, down), range(2)):
        @pl.when(there)
        def _(s=s):
            raw_send(s).start()

    def zero(ref):
        ref[...] = jnp.zeros(ref.shape, ref.dtype)

    def wide(ref, h):
        u = ref.shape[1] - 2
        return dict(ref=ref, h=h, hl=(0, 1), first=(1, 0), last=(u, 1), hr=(u + 1, 0), real=pl.ds(1, u))

    def flat(ref, h):
        w = ref.shape[1] - 2
        return dict(ref=ref, h=h, hl=(0,), first=(1,), last=(w,), hr=(w + 1,), real=pl.ds(1, w))

    bufs = [wide(y1, y1.shape[0] - 2), wide(z1, z1.shape[0] - 2), flat(y2, y2.shape[0] - 2), wide(z2, z2.shape[0] - 2),
            flat(y3, y3.shape[0] - 2)]

    for b in bufs:
        ref, h = b['ref'], b['h']

        @pl.when(jnp.logical_not(up))
        def _(ref=ref):
            zero(ref.at[0])

        @pl.when(jnp.logical_not(down))
        def _(ref=ref, h=h):
            zero(ref.at[h + 1])

        @pl.when(jnp.logical_not(left))
        def _(ref=ref, b=b, h=h):
            for r in range(h + 2):
                zero(ref.at[(r,) + b['hl']])

        @pl.when(jnp.logical_not(right))
        def _(ref=ref, b=b, h=h):
            for r in range(h + 2):
                zero(ref.at[(r,) + b['hr']])

    @pl.when(jnp.logical_not(up))
    def _():
        for n in range(nimg):
            zero(raw.at[0, n, 0])

    @pl.when(jnp.logical_not(down))
    def _():
        for n in range(nimg):
            zero(raw.at[last, n, 1])

    xu = xt.shape[1] - 2

    @pl.when(jnp.logical_not(left))
    def _():
        for k in range(last + 1):
            zero(xt.at[k, 0, 3])

    @pl.when(jnp.logical_not(right))
    def _():
        for k in range(last + 1):
            zero(xt.at[k, xu + 1, 0])

    def row_copy(i, s):
        b = bufs[i]
        ref, h = b['ref'], b['h']
        src, dst, dr = (1, h + 1, -1) if s == 0 else (h, 0, 1)
        return pltpu.make_async_remote_copy(ref.at[src, b['real']], ref.at[dst, b['real']], row_send.at[i, s], row_recv.at[i, s],
                                            device_id=dev(dr, 0), device_id_type=pl.DeviceIdType.MESH)

    def corner_copy(i, s):
        b = bufs[i]
        ref, h = b['ref'], b['h']
        dr, dc = near[4 + s][1:]
        src = (1 if dr < 0 else h,) + (b['first'] if dc < 0 else b['last'])
        dst = (h + 1 if dr < 0 else 0,) + (b['hr'] if dc < 0 else b['hl'])
        return pltpu.make_async_remote_copy(ref.at[src], ref.at[dst], cor_send.at[i, s], cor_recv.at[i, s],
                                            device_id=dev(dr, dc), device_id_type=pl.DeviceIdType.MESH)

    def col_copy(i, r, s):
        b = bufs[i]
        ref = b['ref']
        src, dst, dc = (b['first'], b['hr'], -1) if s == 0 else (b['last'], b['hl'], 1)
        return pltpu.make_async_remote_copy(ref.at[(r + 1,) + src], ref.at[(r + 1,) + dst], col_send.at[i, r, s], col_recv.at[i, r, s],
                                            device_id=dev(0, dc), device_id_type=pl.DeviceIdType.MESH)

    sides = ((left, 0), (right, 1))
    from_sides = ((right, 0), (left, 1))

    def each(cases, act):
        for there, s in cases:
            @pl.when(there)
            def _(s=s):
                act(s)

    def send_cols(i, r):
        each(sides, lambda s: col_copy(i, r, s).start())

    def wait_cols(i, r):
        each(from_sides, lambda s: col_copy(i, r, s).wait_recv())

    ends = list(zip((up, down), range(2)))
    from_ends = list(zip((down, up), range(2)))
    corners = [(x[0], s) for s, x in enumerate(near[4:])]
    from_corners = [(x[0], s) for s, x in enumerate(near[:3:-1])]

    def send_rows(i):
        each(ends, lambda s: row_copy(i, s).start())
        each(corners, lambda s: corner_copy(i, s).start())

    def wait_rows(i):
        each(from_ends, lambda s: row_copy(i, s).wait_recv())
        each(from_corners, lambda s: corner_copy(i, s).wait_recv())

    def xcol_copy(k, s):
        src, dst, dc = ((1, 0), (xu + 1, 0), -1) if s == 0 else ((xu, 3), (0, 3), 1)
        return pltpu.make_async_remote_copy(xt.at[(k,) + src], xt.at[(k,) + dst], xc_send.at[k, s], xc_recv.at[k, s],
                                            device_id=dev(0, dc), device_id_type=pl.DeviceIdType.MESH)

    def send_xcols(k):
        each(sides, lambda s: xcol_copy(k, s).start())

    def wait_xcols(k):
        each(from_sides, lambda s: xcol_copy(k, s).wait_recv())

    for i in (0, 1, 6, 7):
        wcopies[i].wait()
    zb = jnp.zeros((64, LANES), BF)
    for dk in range(2):
        for dc in range(3):
            for cpar in range(2):
                for rpar in range(2):
                    r0 = (dk * 3 + dc) * TILE + (cpar * 2 + rpar) * 64
                    for j in range(2):
                        q = 2 * (dc - j) + cpar
                        wp1[pl.ds(r0, 64), pl.ds(j * LANES, LANES)] = vwd1[2 * dk + rpar, q] if 0 <= q < 4 else zb
    zc = jnp.zeros((LANES, LANES), BF)
    for p in range(3):
        for s in range(4):
            for j in range(2):
                q = s - j
                wp2[pl.ds((p * 4 + s) * LANES, LANES), pl.ds(j * LANES, LANES)] = vwc1[p, q] if 0 <= q < 3 else zc

    eye = (lax.broadcasted_iota(jnp.int32, (LANES, LANES), 0) == lax.broadcasted_iota(jnp.int32, (LANES, LANES), 1)).astype(F32).astype(BF)

    def transpose_in(k, st):
        for s in range(nimg // 2):
            rhs = raw[k, pl.ds(2 * s, 2)].reshape(TILE, LANES)
            t = lax.dot_general(eye, rhs, BY_LAST, preferred_element_type=F32)
            st[pl.ds(2 * s * PITCH, LANES), :] = t[:, :LANES]
            st[pl.ds((2 * s + 1) * PITCH, LANES), :] = t[:, LANES:]

    def transpose_out(k, st):
        for c in range(4 * xu):
            xt[k, 1 + c // 4, c % 4] = st[pl.ds(c, nimg, stride=PITCH), :].astype(BF)

    def middle_out(t):
        h = (t + 1) // 2
        return mid + h * (1 - 2 * (t % 2))

    def take_three(it, carry):
        ks = [middle_out(3 * it + d) for d in range(3)]
        sts = [st0, st1, st2]
        for k in ks:
            raw_copy(k).wait()
        for k, st in zip(ks, sts):
            transpose_in(k, st)
        for k, st in zip(ks, sts):
            transpose_out(k, st)
        for k in ks:
            send_xcols(k)
        return carry

    lax.fori_loop(0, (last - 1) // 3, take_three, 0)

    def take_edges():
        first_copy.wait()
        last_copy.wait()

        each(from_ends, lambda s: raw_send(s).wait_recv())
        transpose_in(0, st0)
        transpose_in(last, st1)
        transpose_out(0, st0)
        transpose_out(last, st1)
        send_xcols(0)
        send_xcols(last)

    def finish(acc, bias):
        return jnp.maximum(acc + bias, 0.0).astype(BF)

    def put_pairs(ref, i, v):
        for j in range(2):
            ref[i + 1, pl.ds(1, pairs), j] = v[:, j * LANES:(j + 1) * LANES].reshape(pairs, nimg, LANES)

    def rows_of(ref, idx, w):
        v = ref[idx]
        return v.reshape(w * nimg, v.shape[-1])

    pairs = y1.shape[1] - 2
    bias1 = jnp.concatenate([vb1[...], vb1[...]], axis=-1)
    h1 = y1.shape[0] - 2

    def down1(t, carry):
        a = h1 // 2 - 1 - t

        @pl.when(t == 0)
        def _():
            wait_xcols(mid)

        @pl.when(t == 4)
        def _():
            take_edges()
        wait_xcols(a)
        wait_xcols(last - a)
        for i in (a, h1 - 1 - a):
            parts = []
            for dk in range(2):
                for p in range(3, 9):
                    parts.append(rows_of(xt, (i + dk, pl.ds(p // 4, pairs), p % 4), pairs))
            acc = jnp.dot(jnp.concatenate(parts, axis=-1), wp1[...], preferred_element_type=F32)
            v = finish(acc, bias1)
            put_pairs(y1, i, v)
        send_cols(0, a)
        send_cols(0, h1 - 1 - a)
        return carry

    lax.fori_loop(0, h1 // 2, down1, 0)
    send_rows(0)

    def wait_conv(i, a, h):
        @pl.when(a == h // 2 - 1)
        def _():
            wait_cols(i, a)
            wait_cols(i, h - 1 - a)

        @pl.when(a > 0)
        def _():
            wait_cols(i, a - 1)
            wait_cols(i, h - a)

        @pl.when(a == 0)
        def _():
            wait_rows(i)

    def wait_down(i, a, h):
        hs = 2 * h

        @pl.when(a == h // 2 - 1)
        def _():
            wait_cols(i, 2 * a + 1)
            wait_cols(i, hs - 2 - 2 * a)
        wait_cols(i, 2 * a)
        wait_cols(i, hs - 1 - 2 * a)

        @pl.when(a > 0)
        def _():
            wait_cols(i, 2 * a - 1)
            wait_cols(i, hs - 2 * a)

        @pl.when(a == 0)
        def _():
            wait_rows(i)

    bias2 = jnp.concatenate([vb2[...], vb2[...]], axis=-1)

    def conv1(t, carry):
        a = h1 // 2 - 1 - t
        wait_conv(0, a, h1)
        for i in (a, h1 - 1 - a):
            parts = []
            for p in range(3):
                for s in range(1, 5):
                    parts.append(rows_of(y1, (i + p, pl.ds(s // 2, pairs), s % 2), pairs))
            acc = jnp.dot(jnp.concatenate(parts, axis=-1), wp2[...], preferred_element_type=F32)
            v = finish(acc, bias2)
            put_pairs(z1, i, v)
        send_cols(1, a)
        send_cols(1, h1 - 1 - a)
        return carry

    lax.fori_loop(0, h1 // 2, conv1, 0)
    send_rows(1)

    h2 = y2.shape[0] - 2
    w2 = y2.shape[1] - 2
    for i in (2, 8):
        wcopies[i].wait()

    def down2(t, carry):
        a = h2 // 2 - 1 - t
        wait_down(1, a, h2)
        for i in (a, h2 - 1 - a):
            parts = []
            for p in range(4):
                for s in range(1, 5):
                    parts.append(rows_of(z1, (2 * i + p, pl.ds(s // 2, w2), s % 2), w2))
            acc = jnp.dot(jnp.concatenate(parts, axis=-1), vwd2[...].reshape(16 * LANES, TILE), preferred_element_type=F32)
            y2[i + 1, pl.ds(1, w2)] = finish(acc, vb3[...]).reshape(w2, nimg, TILE)
        send_cols(2, a)
        send_cols(2, h2 - 1 - a)
        return carry

    lax.fori_loop(0, h2 // 2, down2, 0)
    send_rows(2)
    for i in (3, 9):
        wcopies[i].wait()

    def conv2(t, carry):
        a = h2 // 2 - 1 - t
        wait_conv(2, a, h2)
        for i in (a, h2 - 1 - a):
            parts = []
            for p in range(3):
                for q in range(3):
                    parts.append(rows_of(y2, (i + p, pl.ds(q, w2)), w2))
            acc = jnp.dot(jnp.concatenate(parts, axis=-1), vwc2[...].reshape(9 * TILE, TILE), preferred_element_type=F32)
            v = finish(acc, vb4[...]).reshape(w2 // 2, 2, nimg, TILE)
            z2[i + 1, pl.ds(1, w2 // 2), 0] = v[:, 0]
            z2[i + 1, pl.ds(1, w2 // 2), 1] = v[:, 1]
        send_cols(3, a)
        send_cols(3, h2 - 1 - a)
        return carry

    lax.fori_loop(0, h2 // 2, conv2, 0)
    send_rows(3)

    h3 = y3.shape[0] - 2
    w3 = y3.shape[1] - 2
    ch3 = out.shape[-1]
    for i in (4, 10, 5, 11):
        wcopies[i].wait()
    wp6[...] = jnp.zeros(wp6.shape, BF)
    for p in range(3):
        for q in range(3):
            wp6[p * 3 + q, pl.ds(0, ch3), :] = vwc3[p, q]

    def down3(t, carry):
        a = h3 // 2 - 1 - t
        wait_down(3, a, h3)
        ii = (a, h3 - 1 - a)
        acc = None
        for p in range(4):
            for s in range(1, 5):
                lhs = jnp.concatenate([rows_of(z2, (2 * i + p, pl.ds(s // 2, w3), s % 2), w3) for i in ii], axis=0)
                d = lax.dot_general(lhs, vwd3[p, s - 1], BY_LAST, preferred_element_type=F32)
                acc = d if acc is None else acc + d
        v = finish(acc, vb5[...])
        v = jnp.concatenate([v, jnp.zeros((v.shape[0], y3.shape[-1] - ch3), BF)], axis=-1)
        for n, i in enumerate(ii):
            y3[i + 1, pl.ds(1, w3)] = v[n * w3 * nimg:(n + 1) * w3 * nimg].reshape(w3, nimg, y3.shape[-1])
        send_cols(4, a)
        send_cols(4, h3 - 1 - a)
        return carry

    lax.fori_loop(0, h3 // 2, down3, 0)
    send_rows(4)

    def conv3(t, carry):
        a = h3 // 2 - 1 - t
        wait_conv(4, a, h3)
        ii = (a, h3 - 1 - a)
        parts = []
        for p in range(3):
            for q in range(3):
                parts.append(jnp.concatenate([rows_of(y3, (i + p, pl.ds(q, w3)), w3) for i in ii], axis=0))
        acc = jnp.dot(jnp.concatenate(parts, axis=-1), wp6[...].reshape(9 * wp6.shape[1], ch3), preferred_element_type=F32)
        v = finish(acc, vb6[...])
        for n, i in enumerate(ii):
            out[i] = v[n * w3 * nimg:(n + 1) * w3 * nimg].reshape(w3, nimg, ch3)
        return carry

    lax.fori_loop(0, h3 // 2, conv3, 0)

    each(ends, lambda s: raw_send(s).wait_send())

    def drain(make, count):
        def one(r, carry):
            make(r).wait_send()
            return carry
        lax.fori_loop(0, count, one, 0)

    each(sides, lambda s: drain(lambda k: xcol_copy(k, s), last + 1))
    for i, b in enumerate(bufs):
        each(ends, lambda s: row_copy(i, s).wait_send())
        each(corners, lambda s: corner_copy(i, s).wait_send())
        each(sides, lambda s: drain(lambda r: col_copy(i, r, s), b['h']))


def solution(mesh):
    dims = (mesh.shape['row'], mesh.shape['col'])

    def local_encoder(images, w_down1, b_down1, w_conv1, b_conv1, w_down2, b_down2, w_conv2, b_conv2, w_down3, b_down3, w_conv3, b_conv3):
        n, h, w, c = images.shape
        img = jnp.transpose(images, (0, 1, 3, 2))
        wd3 = jnp.transpose(w_down3, (0, 1, 3, 2))
        c1, c2, c3 = w_conv1.shape[-1], w_conv2.shape[-1], w_conv3.shape[-1]
        c3p = pl.cdiv(c3, LANES) * LANES
        hbm = pl.BlockSpec(memory_space=pl.ANY)
        dma = pltpu.SemaphoreType.DMA
        hh, hq, he = h // 2, h // 4, h // 8
        wq, we = w // 4, w // 8
        kk = hh + 1
        scratch = [
            pltpu.VMEM((kk, n, 2, c, w), BF),
            pltpu.VMEM((kk, wq + 2, 4, n, 2 * c), BF),
            pltpu.VMEM((hh + 2, wq + 2, 2, n, c1), BF),
            pltpu.VMEM((hh + 2, wq + 2, 2, n, c1), BF),
            pltpu.VMEM((hq + 2, wq + 2, n, c2), BF),
            pltpu.VMEM((hq + 2, we + 2, 2, n, c2), BF),
            pltpu.VMEM((he + 2, we + 2, n, c3p), BF),
        ] + [pltpu.VMEM((n * PITCH, LANES), F32)] * 3 + [
            pltpu.VMEM(x.shape, BF) for x in (w_down1, w_conv1, w_down2, w_conv2, wd3, w_conv3)
        ] + [
            pltpu.VMEM((6 * TILE, TILE), BF),
            pltpu.VMEM((6 * TILE, TILE), BF),
            pltpu.VMEM((9, c3p, c3), BF),
        ] + [pltpu.VMEM((1, k), F32) for k in (c1, c1, c2, c2, c3, c3)] + [
            dma(d) for d in ((kk,), (12,), (2,), (2,), (kk, 2), (kk, 2), (5, 2), (5, 2), (5, 4), (5, 4), (5, hh, 2), (5, hh, 2))
        ]
        biases = [b.reshape(1, -1) for b in (b_down1, b_conv1, b_down2, b_conv2, b_down3, b_conv3)]
        feats = pl.pallas_call(
            functools.partial(_encoder_kernel, dims),
            out_shape=jax.ShapeDtypeStruct((he, we, n, c3), BF),
            in_specs=[hbm] * 13,
            out_specs=pl.BlockSpec(memory_space=pltpu.VMEM),
            scratch_shapes=scratch,
            compiler_params=pltpu.CompilerParams(collective_id=0, has_side_effects=True, vmem_limit_bytes=62 * 1024 * 1024),
        )(img, w_down1, biases[0], w_conv1, biases[1], w_down2, biases[2], w_conv2, biases[3], wd3, biases[4], w_conv3, biases[5])
        return jnp.transpose(feats, (2, 0, 1, 3))

    tile_spec = P('batch', 'row', 'col', None)
    return jax.shard_map(local_encoder, mesh=mesh, in_specs=(tile_spec,) + (P(),) * 12, out_specs=tile_spec, check_vma=False)
```

```python
import functools

import jax
import jax.numpy as jnp
from jax import lax
from jax.experimental import pallas as pl
from jax.experimental.pallas import tpu as pltpu
from jax.sharding import PartitionSpec as P

BY_LAST = (((1,), (1,)), ((), ()))
BF = jnp.bfloat16
F32 = jnp.float32
LANES = 128
TILE = 2 * LANES
PITCH = 129


def _encoder_kernel(dims, img, wd1, bd1, wc1, bc1, wd2, bd2, wc2, bc2, wd3, bd3, wc3, bc3, out,
                    raw, xt, y1, z1, y2, z2, y3, st0, st1, st2,
                    vwd1, vwc1, vwd2, vwc2, vwd3, vwc3, wp1, wp2, wp6,
                    vb1, vb2, vb3, vb4, vb5, vb6,
                    raw_sem, w_sem, rh_send, rh_recv, xc_send, xc_recv,
                    row_send, row_recv, cor_send, cor_recv, col_send, col_recv):
    row_len, col_len = dims
    nimg = img.shape[0]
    my_row = lax.axis_index('row')
    my_col = lax.axis_index('col')
    up, down = my_row > 0, my_row < row_len - 1
    left, right = my_col > 0, my_col < col_len - 1

    def both(a, b):
        return jnp.logical_and(a, b)

    near = [(up, -1, 0), (down, 1, 0), (left, 0, -1), (right, 0, 1)]
    near += [(both(v[0], g[0]), v[1], g[2]) for v in near[:2] for g in near[2:]]

    def dev(dr, dc):
        return {'row': my_row + dr, 'col': my_col + dc}

    def raw_copy(k):
        return pltpu.make_async_copy(img.at[:, pl.ds(2 * k - 1, 2)], raw.at[k], raw_sem.at[k])

    last = raw.shape[0] - 1
    mid = last // 2
    first_copy = pltpu.make_async_copy(img.at[:, pl.ds(0, 1)], raw.at[0, :, pl.ds(1, 1)], raw_sem.at[0])
    last_copy = pltpu.make_async_copy(img.at[:, pl.ds(2 * last - 1, 1)], raw.at[last, :, pl.ds(0, 1)], raw_sem.at[last])
    order = []
    for t in range(last - 1):
        h = (t + 1) // 2
        order.append(mid - h if t % 2 else mid + h)
    weights = [(wd1, vwd1), (wc1, vwc1), (wd2, vwd2), (wc2, vwc2), (wd3, vwd3), (wc3, vwc3),
               *((x, v.at[0]) for x, v in zip((bd1, bc1, bd2, bc2, bd3, bc3), (vb1, vb2, vb3, vb4, vb5, vb6)))]
    wcopies = [pltpu.make_async_copy(s, d, w_sem.at[i]) for i, (s, d) in enumerate(weights)]
    for i in (0, 6, 1, 7):
        wcopies[i].start()
    for k in order:
        raw_copy(k).start()
    first_copy.start()
    last_copy.start()
    for i in (2, 8, 3, 9, 4, 10, 5, 11):
        wcopies[i].start()

    barrier = pltpu.get_barrier_semaphore()
    for there, dr, dc in near:
        @pl.when(there)
        def _(dr=dr, dc=dc):
            pl.semaphore_signal(barrier, inc=1, device_id=dev(dr, dc), device_id_type=pl.DeviceIdType.MESH)
    nu, nd, nl, nr = [jnp.where(x, 1, 0) for x in (up, down, left, right)]
    pl.semaphore_wait(barrier, (1 + nu + nd) * (1 + nl + nr) - 1)

    def raw_send(s):
        if s == 0:
            return pltpu.make_async_remote_copy(img.at[:, pl.ds(0, 1)], raw.at[last, :, pl.ds(1, 1)],
                                                rh_send.at[0], rh_recv.at[0], device_id=dev(-1, 0), device_id_type=pl.DeviceIdType.MESH)
        return pltpu.make_async_remote_copy(img.at[:, pl.ds(2 * last - 1, 1)], raw.at[0, :, pl.ds(0, 1)],
                                            rh_send.at[1], rh_recv.at[1], device_id=dev(1, 0), device_id_type=pl.DeviceIdType.MESH)

    for there, s in zip((up, down), range(2)):
        @pl.when(there)
        def _(s=s):
            raw_send(s).start()

    def zero(ref):
        ref[...] = jnp.zeros(ref.shape, ref.dtype)

    def wide(ref, h):
        u = ref.shape[1] - 2
        return dict(ref=ref, h=h, hl=(0, 1), first=(1, 0), last=(u, 1), hr=(u + 1, 0), real=pl.ds(1, u))

    def flat(ref, h):
        w = ref.shape[1] - 2
        return dict(ref=ref, h=h, hl=(0,), first=(1,), last=(w,), hr=(w + 1,), real=pl.ds(1, w))

    bufs = [wide(y1, y1.shape[0] - 2), wide(z1, z1.shape[0] - 2), flat(y2, y2.shape[0] - 2), wide(z2, z2.shape[0] - 2),
            flat(y3, y3.shape[0] - 2)]

    for b in bufs:
        ref, h = b['ref'], b['h']

        @pl.when(jnp.logical_not(up))
        def _(ref=ref):
            zero(ref.at[0])

        @pl.when(jnp.logical_not(down))
        def _(ref=ref, h=h):
            zero(ref.at[h + 1])

        @pl.when(jnp.logical_not(left))
        def _(ref=ref, b=b, h=h):
            for r in range(h + 2):
                zero(ref.at[(r,) + b['hl']])

        @pl.when(jnp.logical_not(right))
        def _(ref=ref, b=b, h=h):
            for r in range(h + 2):
                zero(ref.at[(r,) + b['hr']])

    @pl.when(jnp.logical_not(up))
    def _():
        for n in range(nimg):
            zero(raw.at[0, n, 0])

    @pl.when(jnp.logical_not(down))
    def _():
        for n in range(nimg):
            zero(raw.at[last, n, 1])

    xu = xt.shape[1] - 2

    @pl.when(jnp.logical_not(left))
    def _():
        for k in range(last + 1):
            zero(xt.at[k, 0, 3])

    @pl.when(jnp.logical_not(right))
    def _():
        for k in range(last + 1):
            zero(xt.at[k, xu + 1, 0])

    def row_copy(i, s):
        b = bufs[i]
        ref, h = b['ref'], b['h']
        src, dst, dr = (1, h + 1, -1) if s == 0 else (h, 0, 1)
        return pltpu.make_async_remote_copy(ref.at[src, b['real']], ref.at[dst, b['real']], row_send.at[i, s], row_recv.at[i, s],
                                            device_id=dev(dr, 0), device_id_type=pl.DeviceIdType.MESH)

    def corner_copy(i, s):
        b = bufs[i]
        ref, h = b['ref'], b['h']
        dr, dc = near[4 + s][1:]
        src = (1 if dr < 0 else h,) + (b['first'] if dc < 0 else b['last'])
        dst = (h + 1 if dr < 0 else 0,) + (b['hr'] if dc < 0 else b['hl'])
        return pltpu.make_async_remote_copy(ref.at[src], ref.at[dst], cor_send.at[i, s], cor_recv.at[i, s],
                                            device_id=dev(dr, dc), device_id_type=pl.DeviceIdType.MESH)

    def col_copy(i, r, s):
        b = bufs[i]
        ref = b['ref']
        src, dst, dc = (b['first'], b['hr'], -1) if s == 0 else (b['last'], b['hl'], 1)
        return pltpu.make_async_remote_copy(ref.at[(r + 1,) + src], ref.at[(r + 1,) + dst], col_send.at[i, r, s], col_recv.at[i, r, s],
                                            device_id=dev(0, dc), device_id_type=pl.DeviceIdType.MESH)

    sides = ((left, 0), (right, 1))
    from_sides = ((right, 0), (left, 1))

    def each(cases, act):
        for there, s in cases:
            @pl.when(there)
            def _(s=s):
                act(s)

    def send_cols(i, r):
        each(sides, lambda s: col_copy(i, r, s).start())

    def wait_cols(i, r):
        each(from_sides, lambda s: col_copy(i, r, s).wait_recv())

    ends = list(zip((up, down), range(2)))
    from_ends = list(zip((down, up), range(2)))
    corners = [(x[0], s) for s, x in enumerate(near[4:])]
    from_corners = [(x[0], s) for s, x in enumerate(near[:3:-1])]

    def send_rows(i):
        each(ends, lambda s: row_copy(i, s).start())
        each(corners, lambda s: corner_copy(i, s).start())

    def wait_rows(i):
        each(from_ends, lambda s: row_copy(i, s).wait_recv())
        each(from_corners, lambda s: corner_copy(i, s).wait_recv())

    def xcol_copy(k, s):
        src, dst, dc = ((1, 0), (xu + 1, 0), -1) if s == 0 else ((xu, 3), (0, 3), 1)
        return pltpu.make_async_remote_copy(xt.at[(k,) + src], xt.at[(k,) + dst], xc_send.at[k, s], xc_recv.at[k, s],
                                            device_id=dev(0, dc), device_id_type=pl.DeviceIdType.MESH)

    def send_xcols(k):
        each(sides, lambda s: xcol_copy(k, s).start())

    def wait_xcols(k):
        each(from_sides, lambda s: xcol_copy(k, s).wait_recv())

    for i in (0, 1, 6, 7):
        wcopies[i].wait()
    zb = jnp.zeros((64, LANES), BF)
    for dk in range(2):
        for dc in range(3):
            for cpar in range(2):
                for rpar in range(2):
                    r0 = (dk * 3 + dc) * TILE + (cpar * 2 + rpar) * 64
                    for j in range(2):
                        q = 2 * (dc - j) + cpar
                        wp1[pl.ds(r0, 64), pl.ds(j * LANES, LANES)] = vwd1[2 * dk + rpar, q] if 0 <= q < 4 else zb
    zc = jnp.zeros((LANES, LANES), BF)
    for p in range(3):
        for s in range(4):
            for j in range(2):
                q = s - j
                wp2[pl.ds((p * 4 + s) * LANES, LANES), pl.ds(j * LANES, LANES)] = vwc1[p, q] if 0 <= q < 3 else zc

    eye = (lax.broadcasted_iota(jnp.int32, (LANES, LANES), 0) == lax.broadcasted_iota(jnp.int32, (LANES, LANES), 1)).astype(F32).astype(BF)

    def transpose_in(k, st):
        for s in range(nimg // 2):
            rhs = raw[k, pl.ds(2 * s, 2)].reshape(TILE, LANES)
            t = lax.dot_general(eye, rhs, BY_LAST, preferred_element_type=F32)
            st[pl.ds(2 * s * PITCH, LANES), :] = t[:, :LANES]
            st[pl.ds((2 * s + 1) * PITCH, LANES), :] = t[:, LANES:]

    def transpose_out(k, st):
        for c in range(4 * xu):
            xt[k, 1 + c // 4, c % 4] = st[pl.ds(c, nimg, stride=PITCH), :].astype(BF)

    def middle_out(t):
        h = (t + 1) // 2
        return mid + h * (1 - 2 * (t % 2))

    def take_three(it, carry):
        ks = [middle_out(3 * it + d) for d in range(3)]
        sts = [st0, st1, st2]
        for k in ks:
            raw_copy(k).wait()
        for k, st in zip(ks, sts):
            transpose_in(k, st)
        for k, st in zip(ks, sts):
            transpose_out(k, st)
        for k in ks:
            send_xcols(k)
        return carry

    lax.fori_loop(0, (last - 1) // 3, take_three, 0)

    def take_edges():
        first_copy.wait()
        last_copy.wait()

        each(from_ends, lambda s: raw_send(s).wait_recv())
        transpose_in(0, st0)
        transpose_in(last, st1)
        transpose_out(0, st0)
        transpose_out(last, st1)
        send_xcols(0)
        send_xcols(last)

    def finish(acc, bias):
        return jnp.maximum(acc + bias, 0.0).astype(BF)

    def put_pairs(ref, i, v):
        for j in range(2):
            ref[i + 1, pl.ds(1, pairs), j] = v[:, j * LANES:(j + 1) * LANES].reshape(pairs, nimg, LANES)

    def rows_of(ref, idx, w):
        v = ref[idx]
        return v.reshape(w * nimg, v.shape[-1])

    def wait_pair(i, a, h):
        wait_cols(i, a)
        wait_cols(i, h - 1 - a)

    def wait_conv(i, t, a, h, e):
        n = h // 2

        @pl.when(t == (0 if e else 1))
        def _():
            wait_pair(i, n - 1, h)

        @pl.when(jnp.logical_or(t < e, a >= 3))
        def _():
            wait_pair(i, a - 1, h)

        @pl.when(t == e)
        def _():
            for s in range(min(2, n - e - 1)):
                wait_pair(i, s, h)
            wait_rows(i)

    def wait_down(i, t, a, h, e):
        n = h // 2

        @pl.when(t == (0 if e else 1))
        def _():
            wait_pair(i, h - 1, 2 * h)

        @pl.when(jnp.logical_or(t < e, a >= 2))
        def _():
            wait_pair(i, 2 * a, 2 * h)
            wait_pair(i, 2 * a - 1, 2 * h)

        @pl.when(t == e)
        def _():
            for s in range(min(3, 2 * (n - e) - 1)):
                wait_pair(i, s, 2 * h)
            wait_rows(i)

    def send(i, t, a, h, e):
        send_cols(i, a)
        send_cols(i, h - 1 - a)

        @pl.when(t == e)
        def _():
            send_rows(i)

    def step_of(t, n, e):
        if not e:
            return lax.rem(n - t, n)
        past = (t + n - 1 - e) // n
        return n - 1 - t + past - (n - 1 - e) * ((t + n - e) // n - past)

    pairs = y1.shape[1] - 2
    bias1 = jnp.concatenate([vb1[...], vb1[...]], axis=-1)
    h1 = y1.shape[0] - 2

    e1 = 4

    def down1(t, carry):
        a = step_of(t, h1 // 2, e1)

        @pl.when(t == 0)
        def _():
            wait_xcols(mid)

        @pl.when(t == 1)
        def _():
            take_edges()

        @pl.when(jnp.logical_or(t < e1, a >= 2))
        def _():
            wait_xcols(a)
            wait_xcols(last - a)

        @pl.when(t == e1)
        def _():
            for k in (0, 1):
                wait_xcols(k)
                wait_xcols(last - k)
        for i in (a, h1 - 1 - a):
            parts = []
            for dk in range(2):
                for p in range(3, 9):
                    parts.append(rows_of(xt, (i + dk, pl.ds(p // 4, pairs), p % 4), pairs))
            acc = jnp.dot(jnp.concatenate(parts, axis=-1), wp1[...], preferred_element_type=F32)
            v = finish(acc, bias1)
            put_pairs(y1, i, v)
        send(0, t, a, h1, e1)
        return carry

    lax.fori_loop(0, h1 // 2, down1, 0)

    bias2 = jnp.concatenate([vb2[...], vb2[...]], axis=-1)

    def conv1(t, carry):
        a = step_of(t, h1 // 2, 3)
        wait_conv(0, t, a, h1, 3)
        for i in (a, h1 - 1 - a):
            parts = []
            for p in range(3):
                for s in range(1, 5):
                    parts.append(rows_of(y1, (i + p, pl.ds(s // 2, pairs), s % 2), pairs))
            acc = jnp.dot(jnp.concatenate(parts, axis=-1), wp2[...], preferred_element_type=F32)
            v = finish(acc, bias2)
            put_pairs(z1, i, v)
        send(1, t, a, h1, 3)
        return carry

    lax.fori_loop(0, h1 // 2, conv1, 0)

    h2 = y2.shape[0] - 2
    w2 = y2.shape[1] - 2
    for i in (2, 8):
        wcopies[i].wait()

    def down2(t, carry):
        a = step_of(t, h2 // 2, 1)
        wait_down(1, t, a, h2, 1)
        for i in (a, h2 - 1 - a):
            parts = []
            for p in range(4):
                for s in range(1, 5):
                    parts.append(rows_of(z1, (2 * i + p, pl.ds(s // 2, w2), s % 2), w2))
            acc = jnp.dot(jnp.concatenate(parts, axis=-1), vwd2[...].reshape(16 * LANES, TILE), preferred_element_type=F32)
            y2[i + 1, pl.ds(1, w2)] = finish(acc, vb3[...]).reshape(w2, nimg, TILE)
        send(2, t, a, h2, 1)
        return carry

    lax.fori_loop(0, h2 // 2, down2, 0)
    for i in (3, 9):
        wcopies[i].wait()

    def conv2(t, carry):
        a = step_of(t, h2 // 2, 2)
        wait_conv(2, t, a, h2, 2)
        for i in (a, h2 - 1 - a):
            parts = []
            for p in range(3):
                for q in range(3):
                    parts.append(rows_of(y2, (i + p, pl.ds(q, w2)), w2))
            acc = jnp.dot(jnp.concatenate(parts, axis=-1), vwc2[...].reshape(9 * TILE, TILE), preferred_element_type=F32)
            v = finish(acc, vb4[...]).reshape(w2 // 2, 2, nimg, TILE)
            z2[i + 1, pl.ds(1, w2 // 2), 0] = v[:, 0]
            z2[i + 1, pl.ds(1, w2 // 2), 1] = v[:, 1]
        send(3, t, a, h2, 2)
        return carry

    lax.fori_loop(0, h2 // 2, conv2, 0)

    h3 = y3.shape[0] - 2
    w3 = y3.shape[1] - 2
    ch3 = out.shape[-1]
    for i in (4, 10, 5, 11):
        wcopies[i].wait()
    wp6[...] = jnp.zeros(wp6.shape, BF)
    for p in range(3):
        for q in range(3):
            wp6[p * 3 + q, pl.ds(0, ch3), :] = vwc3[p, q]

    def down3(t, carry):
        a = step_of(t, h3 // 2, 1)
        wait_down(3, t, a, h3, 1)
        ii = (a, h3 - 1 - a)
        acc = None
        for p in range(4):
            for s in range(1, 5):
                lhs = jnp.concatenate([rows_of(z2, (2 * i + p, pl.ds(s // 2, w3), s % 2), w3) for i in ii], axis=0)
                d = lax.dot_general(lhs, vwd3[p, s - 1], BY_LAST, preferred_element_type=F32)
                acc = d if acc is None else acc + d
        v = finish(acc, vb5[...])
        v = jnp.concatenate([v, jnp.zeros((v.shape[0], y3.shape[-1] - ch3), BF)], axis=-1)
        for n, i in enumerate(ii):
            y3[i + 1, pl.ds(1, w3)] = v[n * w3 * nimg:(n + 1) * w3 * nimg].reshape(w3, nimg, y3.shape[-1])
        send(4, t, a, h3, 1)
        return carry

    lax.fori_loop(0, h3 // 2, down3, 0)

    def conv3(t, carry):
        a = step_of(t, h3 // 2, 1)
        wait_conv(4, t, a, h3, 1)
        ii = (a, h3 - 1 - a)
        parts = []
        for p in range(3):
            for q in range(3):
                parts.append(jnp.concatenate([rows_of(y3, (i + p, pl.ds(q, w3)), w3) for i in ii], axis=0))
        acc = jnp.dot(jnp.concatenate(parts, axis=-1), wp6[...].reshape(9 * wp6.shape[1], ch3), preferred_element_type=F32)
        v = finish(acc, vb6[...])
        for n, i in enumerate(ii):
            out[i] = v[n * w3 * nimg:(n + 1) * w3 * nimg].reshape(w3, nimg, ch3)
        return carry

    lax.fori_loop(0, h3 // 2, conv3, 0)

    each(ends, lambda s: raw_send(s).wait_send())

    def drain(make, count):
        def one(r, carry):
            make(r).wait_send()
            return carry
        lax.fori_loop(0, count, one, 0)

    each(sides, lambda s: drain(lambda k: xcol_copy(k, s), last + 1))
    for i, b in enumerate(bufs):
        each(ends, lambda s: row_copy(i, s).wait_send())
        each(corners, lambda s: corner_copy(i, s).wait_send())
        each(sides, lambda s: drain(lambda r: col_copy(i, r, s), b['h']))


def solution(mesh):
    dims = (mesh.shape['row'], mesh.shape['col'])

    def local_encoder(images, w_down1, b_down1, w_conv1, b_conv1, w_down2, b_down2, w_conv2, b_conv2, w_down3, b_down3, w_conv3, b_conv3):
        n, h, w, c = images.shape
        img = jnp.transpose(images, (0, 1, 3, 2))
        wd3 = jnp.transpose(w_down3, (0, 1, 3, 2))
        c1, c2, c3 = w_conv1.shape[-1], w_conv2.shape[-1], w_conv3.shape[-1]
        c3p = pl.cdiv(c3, LANES) * LANES
        hbm = pl.BlockSpec(memory_space=pl.ANY)
        dma = pltpu.SemaphoreType.DMA
        hh, hq, he = h // 2, h // 4, h // 8
        wq, we = w // 4, w // 8
        kk = hh + 1
        scratch = [
            pltpu.VMEM((kk, n, 2, c, w), BF),
            pltpu.VMEM((kk, wq + 2, 4, n, 2 * c), BF),
            pltpu.VMEM((hh + 2, wq + 2, 2, n, c1), BF),
            pltpu.VMEM((hh + 2, wq + 2, 2, n, c1), BF),
            pltpu.VMEM((hq + 2, wq + 2, n, c2), BF),
            pltpu.VMEM((hq + 2, we + 2, 2, n, c2), BF),
            pltpu.VMEM((he + 2, we + 2, n, c3p), BF),
        ] + [pltpu.VMEM((n * PITCH, LANES), F32)] * 3 + [
            pltpu.VMEM(x.shape, BF) for x in (w_down1, w_conv1, w_down2, w_conv2, wd3, w_conv3)
        ] + [
            pltpu.VMEM((6 * TILE, TILE), BF),
            pltpu.VMEM((6 * TILE, TILE), BF),
            pltpu.VMEM((9, c3p, c3), BF),
        ] + [pltpu.VMEM((1, k), F32) for k in (c1, c1, c2, c2, c3, c3)] + [
            dma(d) for d in ((kk,), (12,), (2,), (2,), (kk, 2), (kk, 2), (5, 2), (5, 2), (5, 4), (5, 4), (5, hh, 2), (5, hh, 2))
        ]
        feats = pl.pallas_call(
            functools.partial(_encoder_kernel, dims),
            out_shape=jax.ShapeDtypeStruct((he, we, n, c3), BF),
            in_specs=[hbm] * 13,
            out_specs=pl.BlockSpec(memory_space=pltpu.VMEM),
            scratch_shapes=scratch,
            compiler_params=pltpu.CompilerParams(collective_id=0, has_side_effects=True, vmem_limit_bytes=62 * 1024 * 1024),
        )(img, w_down1, b_down1, w_conv1, b_conv1, w_down2, b_down2, w_conv2, b_conv2, wd3, b_down3, w_conv3, b_conv3)
        return jnp.transpose(feats, (2, 0, 1, 3))

    tile_spec = P('batch', 'row', 'col', None)
    return jax.shard_map(local_encoder, mesh=mesh, in_specs=(tile_spec,) + (P(),) * 12, out_specs=tile_spec, check_vma=False)
```

```python
import functools

import jax
import jax.numpy as jnp
from jax import lax
from jax.experimental import pallas as pl
from jax.experimental.pallas import tpu as pltpu
from jax.sharding import PartitionSpec as P

BY_LAST = (((1,), (1,)), ((), ()))
BF = jnp.bfloat16
F32 = jnp.float32
LANES = 128
TILE = 2 * LANES
PITCH = 129


def _encoder_kernel(dims, img, wd1, bd1, wc1, bc1, wd2, bd2, wc2, bc2, wd3, bd3, wc3, bc3, out,
                    raw, xt, y1, z1, y2, z2, y3, st0, st1, st2,
                    vwd1, vwc1, vwd2, vwc2, vwd3, vwc3, wp1, wp2, wp6,
                    vb1, vb2, vb3, vb4, vb5, vb6,
                    raw_sem, w_sem, rh_send, rh_recv, xc_send, xc_recv,
                    row_send, row_recv, cor_send, cor_recv, col_send, col_recv):
    row_len, col_len = dims
    nimg = img.shape[0]
    my_row = lax.axis_index('row')
    my_col = lax.axis_index('col')
    up, down = my_row > 0, my_row < row_len - 1
    left, right = my_col > 0, my_col < col_len - 1

    def both(a, b):
        return jnp.logical_and(a, b)

    near = [(up, -1, 0), (down, 1, 0), (left, 0, -1), (right, 0, 1)]
    near += [(both(v[0], g[0]), v[1], g[2]) for v in near[:2] for g in near[2:]]

    def dev(dr, dc):
        return {'row': my_row + dr, 'col': my_col + dc}

    def raw_copy(k):
        return pltpu.make_async_copy(img.at[:, pl.ds(2 * k - 1, 2)], raw.at[k], raw_sem.at[k])

    last = raw.shape[0] - 1
    mid = last // 2
    first_copy = pltpu.make_async_copy(img.at[:, pl.ds(0, 1)], raw.at[0, :, pl.ds(1, 1)], raw_sem.at[0])
    last_copy = pltpu.make_async_copy(img.at[:, pl.ds(2 * last - 1, 1)], raw.at[last, :, pl.ds(0, 1)], raw_sem.at[last])
    order = []
    for t in range(last - 1):
        h = (t + 1) // 2
        order.append(mid - h if t % 2 else mid + h)
    weights = [(wd1, vwd1), (wc1, vwc1), (wd2, vwd2), (wc2, vwc2), (wd3, vwd3), (wc3, vwc3),
               *((x, v.at[0]) for x, v in zip((bd1, bc1, bd2, bc2, bd3, bc3), (vb1, vb2, vb3, vb4, vb5, vb6)))]
    wcopies = [pltpu.make_async_copy(s, d, w_sem.at[i]) for i, (s, d) in enumerate(weights)]
    for i in (0, 6, 1, 7):
        wcopies[i].start()
    for k in order[:6]:
        raw_copy(k).start()

    barrier = pltpu.get_barrier_semaphore()
    for there, dr, dc in near:
        @pl.when(there)
        def _(dr=dr, dc=dc):
            pl.semaphore_signal(barrier, inc=1, device_id=dev(dr, dc), device_id_type=pl.DeviceIdType.MESH)
    nu, nd, nl, nr = [jnp.where(x, 1, 0) for x in (up, down, left, right)]
    pl.semaphore_wait(barrier, (1 + nu + nd) * (1 + nl + nr) - 1)

    def raw_send(s):
        if s == 0:
            return pltpu.make_async_remote_copy(img.at[:, pl.ds(0, 1)], raw.at[last, :, pl.ds(1, 1)],
                                                rh_send.at[0], rh_recv.at[0], device_id=dev(-1, 0), device_id_type=pl.DeviceIdType.MESH)
        return pltpu.make_async_remote_copy(img.at[:, pl.ds(2 * last - 1, 1)], raw.at[0, :, pl.ds(0, 1)],
                                            rh_send.at[1], rh_recv.at[1], device_id=dev(1, 0), device_id_type=pl.DeviceIdType.MESH)

    for there, s in zip((up, down), range(2)):
        @pl.when(there)
        def _(s=s):
            raw_send(s).start()

    def zero(ref):
        ref[...] = jnp.zeros(ref.shape, ref.dtype)

    def wide(ref, h):
        u = ref.shape[1] - 2
        return dict(ref=ref, h=h, hl=(0, 1), first=(1, 0), last=(u, 1), hr=(u + 1, 0), real=pl.ds(1, u))

    def flat(ref, h):
        w = ref.shape[1] - 2
        return dict(ref=ref, h=h, hl=(0,), first=(1,), last=(w,), hr=(w + 1,), real=pl.ds(1, w))

    bufs = [wide(y1, y1.shape[0] - 2), wide(z1, z1.shape[0] - 2), flat(y2, y2.shape[0] - 2), wide(z2, z2.shape[0] - 2),
            flat(y3, y3.shape[0] - 2)]

    for b in bufs:
        ref, h = b['ref'], b['h']

        @pl.when(jnp.logical_not(up))
        def _(ref=ref):
            zero(ref.at[0])

        @pl.when(jnp.logical_not(down))
        def _(ref=ref, h=h):
            zero(ref.at[h + 1])

        @pl.when(jnp.logical_not(left))
        def _(ref=ref, b=b, h=h):
            for r in range(h + 2):
                zero(ref.at[(r,) + b['hl']])

        @pl.when(jnp.logical_not(right))
        def _(ref=ref, b=b, h=h):
            for r in range(h + 2):
                zero(ref.at[(r,) + b['hr']])

    @pl.when(jnp.logical_not(up))
    def _():
        for n in range(nimg):
            zero(raw.at[0, n, 0])

    @pl.when(jnp.logical_not(down))
    def _():
        for n in range(nimg):
            zero(raw.at[last, n, 1])

    xu = xt.shape[1] - 2

    @pl.when(jnp.logical_not(left))
    def _():
        for k in range(last + 1):
            zero(xt.at[k, 0, 3])

    @pl.when(jnp.logical_not(right))
    def _():
        for k in range(last + 1):
            zero(xt.at[k, xu + 1, 0])

    def row_copy(i, s):
        b = bufs[i]
        ref, h = b['ref'], b['h']
        src, dst, dr = (1, h + 1, -1) if s == 0 else (h, 0, 1)
        return pltpu.make_async_remote_copy(ref.at[src, b['real']], ref.at[dst, b['real']], row_send.at[i, s], row_recv.at[i, s],
                                            device_id=dev(dr, 0), device_id_type=pl.DeviceIdType.MESH)

    def corner_copy(i, s):
        b = bufs[i]
        ref, h = b['ref'], b['h']
        dr, dc = near[4 + s][1:]
        src = (1 if dr < 0 else h,) + (b['first'] if dc < 0 else b['last'])
        dst = (h + 1 if dr < 0 else 0,) + (b['hr'] if dc < 0 else b['hl'])
        return pltpu.make_async_remote_copy(ref.at[src], ref.at[dst], cor_send.at[i, s], cor_recv.at[i, s],
                                            device_id=dev(dr, dc), device_id_type=pl.DeviceIdType.MESH)

    def col_copy(i, r, s):
        b = bufs[i]
        ref = b['ref']
        src, dst, dc = (b['first'], b['hr'], -1) if s == 0 else (b['last'], b['hl'], 1)
        return pltpu.make_async_remote_copy(ref.at[(r + 1,) + src], ref.at[(r + 1,) + dst], col_send.at[i, r, s], col_recv.at[i, r, s],
                                            device_id=dev(0, dc), device_id_type=pl.DeviceIdType.MESH)

    sides = ((left, 0), (right, 1))
    from_sides = ((right, 0), (left, 1))

    def each(cases, act):
        for there, s in cases:
            @pl.when(there)
            def _(s=s):
                act(s)

    def send_cols(i, r):
        each(sides, lambda s: col_copy(i, r, s).start())

    def wait_cols(i, r):
        each(from_sides, lambda s: col_copy(i, r, s).wait_recv())

    ends = list(zip((up, down), range(2)))
    from_ends = list(zip((down, up), range(2)))
    corners = [(x[0], s) for s, x in enumerate(near[4:])]
    from_corners = [(x[0], s) for s, x in enumerate(near[:3:-1])]

    def send_rows(i):
        each(ends, lambda s: row_copy(i, s).start())
        each(corners, lambda s: corner_copy(i, s).start())

    def wait_rows(i):
        each(from_ends, lambda s: row_copy(i, s).wait_recv())
        each(from_corners, lambda s: corner_copy(i, s).wait_recv())

    def xcol_copy(k, s):
        src, dst, dc = ((1, 0), (xu + 1, 0), -1) if s == 0 else ((xu, 3), (0, 3), 1)
        return pltpu.make_async_remote_copy(xt.at[(k,) + src], xt.at[(k,) + dst], xc_send.at[k, s], xc_recv.at[k, s],
                                            device_id=dev(0, dc), device_id_type=pl.DeviceIdType.MESH)

    def send_xcols(k):
        each(sides, lambda s: xcol_copy(k, s).start())

    def wait_xcols(k):
        each(from_sides, lambda s: xcol_copy(k, s).wait_recv())

    for i in (0, 1, 6, 7):
        wcopies[i].wait()
    zb = jnp.zeros((64, LANES), BF)
    for dk in range(2):
        for dc in range(3):
            for cpar in range(2):
                for rpar in range(2):
                    r0 = (dk * 3 + dc) * TILE + (cpar * 2 + rpar) * 64
                    for j in range(2):
                        q = 2 * (dc - j) + cpar
                        wp1[pl.ds(r0, 64), pl.ds(j * LANES, LANES)] = vwd1[2 * dk + rpar, q] if 0 <= q < 4 else zb
    zc = jnp.zeros((LANES, LANES), BF)
    for p in range(3):
        for s in range(4):
            for j in range(2):
                q = s - j
                wp2[pl.ds((p * 4 + s) * LANES, LANES), pl.ds(j * LANES, LANES)] = vwc1[p, q] if 0 <= q < 3 else zc

    eye = (lax.broadcasted_iota(jnp.int32, (LANES, LANES), 0) == lax.broadcasted_iota(jnp.int32, (LANES, LANES), 1)).astype(F32).astype(BF)

    def transpose_in(k, st):
        for s in range(nimg // 2):
            rhs = raw[k, pl.ds(2 * s, 2)].reshape(TILE, LANES)
            t = lax.dot_general(eye, rhs, BY_LAST, preferred_element_type=F32)
            st[pl.ds(2 * s * PITCH, LANES), :] = t[:, :LANES]
            st[pl.ds((2 * s + 1) * PITCH, LANES), :] = t[:, LANES:]

    def transpose_out(k, st):
        for c in range(4 * xu):
            xt[k, 1 + c // 4, c % 4] = st[pl.ds(c, nimg, stride=PITCH), :].astype(BF)

    def middle_out(t):
        h = (t + 1) // 2
        return mid + h * (1 - 2 * (t % 2))

    def take_three(it, carry):
        ks = [middle_out(3 * it + d) for d in range(3)]

        @pl.when(it < 3)
        def _():
            for d in range(3):
                raw_copy(middle_out(3 * it + 6 + d)).start()

        @pl.when(it == 3)
        def _():
            first_copy.start()
            last_copy.start()
        sts = [st0, st1, st2]
        for k in ks:
            raw_copy(k).wait()
        for k, st in zip(ks, sts):
            transpose_in(k, st)
        for k, st in zip(ks, sts):
            transpose_out(k, st)
        for k in ks:
            send_xcols(k)
        return carry

    lax.fori_loop(0, (last - 1) // 3, take_three, 0)
    for i in range(2, 6):
        wcopies[i].start()
        wcopies[i + 6].start()

    def take_edges():
        first_copy.wait()
        last_copy.wait()

        each(from_ends, lambda s: raw_send(s).wait_recv())
        transpose_in(0, st0)
        transpose_in(last, st1)
        transpose_out(0, st0)
        transpose_out(last, st1)
        send_xcols(0)
        send_xcols(last)

    def finish(acc, bias):
        return jnp.maximum(acc + bias, 0.0).astype(BF)

    def put_pairs(ref, i, v):
        for j in range(2):
            ref[i + 1, pl.ds(1, pairs), j] = v[:, j * LANES:(j + 1) * LANES].reshape(pairs, nimg, LANES)

    def rows_of(ref, idx, w):
        v = ref[idx]
        return v.reshape(w * nimg, v.shape[-1])

    def wait_pair(i, a, h):
        wait_cols(i, a)
        wait_cols(i, h - 1 - a)

    def step_of(t, n, p):
        up_now = (t + n - p) // n
        return (1 - up_now) * (n - 1 - t) + up_now * (t - p)

    def wait_conv(i, t, a, h, p):
        n = h // 2
        seen = n - 1 - p if p else n

        if p:
            @pl.when(t == 0)
            def _():
                wait_pair(i, n - 1, h)

            @pl.when(t < p)
            def _():
                wait_pair(i, a - 1, h)

        @pl.when(t == p)
        def _():
            wait_pair(i, 0, h)
            wait_rows(i)

        @pl.when(jnp.logical_and(t >= p, a + 1 < seen))
        def _():
            wait_pair(i, a + 1, h)

    def wait_down(i, a, h):
        @pl.when(a == 0)
        def _():
            wait_pair(i, 0, 2 * h)
            wait_rows(i)
        wait_pair(i, 2 * a + 1, 2 * h)

        @pl.when(a < h // 2 - 1)
        def _():
            wait_pair(i, 2 * a + 2, 2 * h)

    def send(i, t, a, h, e):
        send_cols(i, a)
        send_cols(i, h - 1 - a)

        @pl.when(t == e)
        def _():
            send_rows(i)

    pairs = y1.shape[1] - 2
    bias1 = jnp.concatenate([vb1[...], vb1[...]], axis=-1)
    h1 = y1.shape[0] - 2

    e1 = 4

    def down1(t, carry):
        a = step_of(t, h1 // 2, e1)

        @pl.when(t == 0)
        def _():
            wait_xcols(mid)

        @pl.when(t == e1 - 2)
        def _():
            take_edges()

        @pl.when(t < e1)
        def _():
            wait_xcols(a)
            wait_xcols(last - a)

        @pl.when(t == e1)
        def _():
            wait_xcols(0)
            wait_xcols(last)

        @pl.when(jnp.logical_and(t >= e1, a + 1 < h1 // 2 - e1))
        def _():
            wait_xcols(a + 1)
            wait_xcols(last - 1 - a)
        for i in (a, h1 - 1 - a):
            parts = []
            for dk in range(2):
                for p in range(3, 9):
                    parts.append(rows_of(xt, (i + dk, pl.ds(p // 4, pairs), p % 4), pairs))
            acc = jnp.dot(jnp.concatenate(parts, axis=-1), wp1[...], preferred_element_type=F32)
            v = finish(acc, bias1)
            put_pairs(y1, i, v)
        send(0, t, a, h1, e1)
        return carry

    lax.fori_loop(0, h1 // 2, down1, 0)

    bias2 = jnp.concatenate([vb2[...], vb2[...]], axis=-1)

    def conv1(t, carry):
        a = step_of(t, h1 // 2, 2)
        wait_conv(0, t, a, h1, 2)
        for i in (a, h1 - 1 - a):
            parts = []
            for p in range(3):
                for s in range(1, 5):
                    parts.append(rows_of(y1, (i + p, pl.ds(s // 2, pairs), s % 2), pairs))
            acc = jnp.dot(jnp.concatenate(parts, axis=-1), wp2[...], preferred_element_type=F32)
            v = finish(acc, bias2)
            put_pairs(z1, i, v)
        send(1, t, a, h1, 2)
        return carry

    lax.fori_loop(0, h1 // 2, conv1, 0)

    ch3 = out.shape[-1]
    h2 = y2.shape[0] - 2
    w2 = y2.shape[1] - 2
    for i in (2, 8):
        wcopies[i].wait()

    def down2(t, carry):
        a = t
        wait_down(1, a, h2)
        for i in (a, h2 - 1 - a):
            parts = []
            for p in range(4):
                for s in range(1, 5):
                    parts.append(rows_of(z1, (2 * i + p, pl.ds(s // 2, w2), s % 2), w2))
            acc = jnp.dot(jnp.concatenate(parts, axis=-1), vwd2[...].reshape(16 * LANES, TILE), preferred_element_type=F32)
            y2[i + 1, pl.ds(1, w2)] = finish(acc, vb3[...]).reshape(w2, nimg, TILE)
        send(2, t, a, h2, 0)
        return carry

    lax.fori_loop(0, h2 // 2, down2, 0)
    for i in (3, 9, 5):
        wcopies[i].wait()
    wp6[...] = jnp.zeros(wp6.shape, BF)
    for p in range(3):
        for q in range(3):
            wp6[p * 3 + q, pl.ds(0, ch3), :] = vwc3[p, q]

    def conv2(t, carry):
        a = t
        wait_conv(2, t, a, h2, 0)
        for i in (a, h2 - 1 - a):
            parts = []
            for p in range(3):
                for q in range(3):
                    parts.append(rows_of(y2, (i + p, pl.ds(q, w2)), w2))
            acc = jnp.dot(jnp.concatenate(parts, axis=-1), vwc2[...].reshape(9 * TILE, TILE), preferred_element_type=F32)
            v = finish(acc, vb4[...]).reshape(w2 // 2, 2, nimg, TILE)
            z2[i + 1, pl.ds(1, w2 // 2), 0] = v[:, 0]
            z2[i + 1, pl.ds(1, w2 // 2), 1] = v[:, 1]
        send(3, t, a, h2, 0)
        return carry

    lax.fori_loop(0, h2 // 2, conv2, 0)

    h3 = y3.shape[0] - 2
    w3 = y3.shape[1] - 2
    for i in (4, 10, 11):
        wcopies[i].wait()

    def down3(t, carry):
        a = t
        wait_down(3, a, h3)
        ii = (a, h3 - 1 - a)
        acc = None
        for p in range(4):
            for s in range(1, 5):
                lhs = jnp.concatenate([rows_of(z2, (2 * i + p, pl.ds(s // 2, w3), s % 2), w3) for i in ii], axis=0)
                d = lax.dot_general(lhs, vwd3[p, s - 1], BY_LAST, preferred_element_type=F32)
                acc = d if acc is None else acc + d
        v = finish(acc, vb5[...])
        v = jnp.concatenate([v, jnp.zeros((v.shape[0], y3.shape[-1] - ch3), BF)], axis=-1)
        for n, i in enumerate(ii):
            y3[i + 1, pl.ds(1, w3)] = v[n * w3 * nimg:(n + 1) * w3 * nimg].reshape(w3, nimg, y3.shape[-1])
        send(4, t, a, h3, 0)
        return carry

    lax.fori_loop(0, h3 // 2, down3, 0)

    inner = [(i, 1, w3 - 2) for i in range(1, h3 - 1)]
    border = [(0, 0, w3), (h3 - 1, 0, w3)] + [(i, c, 1) for i in range(1, h3 - 1) for c in (0, w3 - 1)]

    def conv3(strips):
        parts = []
        for p in range(3):
            for q in range(3):
                parts.append(jnp.concatenate([rows_of(y3, (i + p, pl.ds(c + q, w)), w) for i, c, w in strips], axis=0))
        acc = jnp.dot(jnp.concatenate(parts, axis=-1), wp6[...].reshape(9 * wp6.shape[1], ch3), preferred_element_type=F32)
        v = finish(acc, vb6[...])
        at = 0
        for i, c, w in strips:
            out[i, pl.ds(c, w)] = v[at:at + w * nimg].reshape(w, nimg, ch3)
            at += w * nimg

    conv3(inner)
    for r in range(h3):
        wait_cols(4, r)
    wait_rows(4)
    conv3(border)

    each(ends, lambda s: raw_send(s).wait_send())

    def drain(make, count):
        def one(r, carry):
            make(r).wait_send()
            return carry
        lax.fori_loop(0, count, one, 0)

    each(sides, lambda s: drain(lambda k: xcol_copy(k, s), last + 1))
    for i, b in enumerate(bufs):
        each(ends, lambda s: row_copy(i, s).wait_send())
        each(corners, lambda s: corner_copy(i, s).wait_send())
        each(sides, lambda s: drain(lambda r: col_copy(i, r, s), b['h']))


def solution(mesh):
    dims = (mesh.shape['row'], mesh.shape['col'])

    def local_encoder(images, w_down1, b_down1, w_conv1, b_conv1, w_down2, b_down2, w_conv2, b_conv2, w_down3, b_down3, w_conv3, b_conv3):
        n, h, w, c = images.shape
        img = jnp.transpose(images, (0, 1, 3, 2))
        wd3 = jnp.transpose(w_down3, (0, 1, 3, 2))
        c1, c2, c3 = w_conv1.shape[-1], w_conv2.shape[-1], w_conv3.shape[-1]
        c3p = pl.cdiv(c3, LANES) * LANES
        hbm = pl.BlockSpec(memory_space=pl.ANY)
        dma = pltpu.SemaphoreType.DMA
        hh, hq, he = h // 2, h // 4, h // 8
        wq, we = w // 4, w // 8
        kk = hh + 1
        scratch = [
            pltpu.VMEM((kk, n, 2, c, w), BF),
            pltpu.VMEM((kk, wq + 2, 4, n, 2 * c), BF),
            pltpu.VMEM((hh + 2, wq + 2, 2, n, c1), BF),
            pltpu.VMEM((hh + 2, wq + 2, 2, n, c1), BF),
            pltpu.VMEM((hq + 2, wq + 2, n, c2), BF),
            pltpu.VMEM((hq + 2, we + 2, 2, n, c2), BF),
            pltpu.VMEM((he + 2, we + 2, n, c3p), BF),
        ] + [pltpu.VMEM((n * PITCH, LANES), F32)] * 3 + [
            pltpu.VMEM(x.shape, BF) for x in (w_down1, w_conv1, w_down2, w_conv2, wd3, w_conv3)
        ] + [
            pltpu.VMEM((6 * TILE, TILE), BF),
            pltpu.VMEM((6 * TILE, TILE), BF),
            pltpu.VMEM((9, c3p, c3), BF),
        ] + [pltpu.VMEM((1, k), F32) for k in (c1, c1, c2, c2, c3, c3)] + [
            dma(d) for d in ((kk,), (12,), (2,), (2,), (kk, 2), (kk, 2), (5, 2), (5, 2), (5, 4), (5, 4), (5, hh, 2), (5, hh, 2))
        ]
        feats = pl.pallas_call(
            functools.partial(_encoder_kernel, dims),
            out_shape=jax.ShapeDtypeStruct((he, we, n, c3), BF),
            in_specs=[hbm] * 13,
            out_specs=pl.BlockSpec(memory_space=pltpu.VMEM),
            scratch_shapes=scratch,
            compiler_params=pltpu.CompilerParams(collective_id=0, has_side_effects=True, vmem_limit_bytes=62 * 1024 * 1024),
        )(img, w_down1, b_down1, w_conv1, b_conv1, w_down2, b_down2, w_conv2, b_conv2, wd3, b_down3, w_conv3, b_conv3)
        return jnp.transpose(feats, (2, 0, 1, 3))

    tile_spec = P('batch', 'row', 'col', None)
    return jax.shard_map(local_encoder, mesh=mesh, in_specs=(tile_spec,) + (P(),) * 12, out_specs=tile_spec, check_vma=False)
```

```python
import functools

import jax
import jax.numpy as jnp
from jax import lax
from jax.experimental import pallas as pl
from jax.experimental.pallas import tpu as pltpu
from jax.sharding import PartitionSpec as P

BY_LAST = (((1,), (1,)), ((), ()))
BF = jnp.bfloat16
F32 = jnp.float32
LANES = 128
TILE = 2 * LANES
PITCH = 129


def _encoder_kernel(dims, img, wd1, bd1, wc1, bc1, wd2, bd2, wc2, bc2, wd3, bd3, wc3, bc3, out,
                    raw, xt, y1, z1, y2, z2, y3, st0, st1, st2,
                    vwd1, vwc1, vwd2, vwc2, vwd3, vwc3, wp1, wp2, wp6,
                    vb1, vb2, vb3, vb4, vb5, vb6,
                    raw_sem, w_sem, rh_send, rh_recv, xc_send, xc_recv,
                    row_send, row_recv, cor_send, cor_recv, col_send, col_recv):
    row_len, col_len = dims
    nimg = img.shape[0]
    my_row = lax.axis_index('row')
    my_col = lax.axis_index('col')
    up, down = my_row > 0, my_row < row_len - 1
    left, right = my_col > 0, my_col < col_len - 1

    def both(a, b):
        return jnp.logical_and(a, b)

    near = [(up, -1, 0), (down, 1, 0), (left, 0, -1), (right, 0, 1)]
    near += [(both(v[0], g[0]), v[1], g[2]) for v in near[:2] for g in near[2:]]

    def dev(dr, dc):
        return {'row': my_row + dr, 'col': my_col + dc}

    def raw_copy(k):
        return pltpu.make_async_copy(img.at[:, pl.ds(2 * k - 1, 2)], raw.at[k], raw_sem.at[k])

    last = raw.shape[0] - 1
    mid = last // 2
    first_copy = pltpu.make_async_copy(img.at[:, pl.ds(0, 1)], raw.at[0, :, pl.ds(1, 1)], raw_sem.at[0])
    last_copy = pltpu.make_async_copy(img.at[:, pl.ds(2 * last - 1, 1)], raw.at[last, :, pl.ds(0, 1)], raw_sem.at[last])
    order = []
    for t in range(last - 1):
        h = (t + 1) // 2
        order.append(mid - h if t % 2 else mid + h)
    weights = [(wd1, vwd1), (wc1, vwc1), (wd2, vwd2), (wc2, vwc2), (wd3, vwd3), (wc3, vwc3),
               *((x, v.at[0]) for x, v in zip((bd1, bc1, bd2, bc2, bd3, bc3), (vb1, vb2, vb3, vb4, vb5, vb6)))]
    wcopies = [pltpu.make_async_copy(s, d, w_sem.at[i]) for i, (s, d) in enumerate(weights)]
    for i in (0, 6, 1, 7):
        wcopies[i].start()
    for k in order[:6]:
        raw_copy(k).start()

    barrier = pltpu.get_barrier_semaphore()
    for there, dr, dc in near:
        @pl.when(there)
        def _(dr=dr, dc=dc):
            pl.semaphore_signal(barrier, inc=1, device_id=dev(dr, dc), device_id_type=pl.DeviceIdType.MESH)
    nu, nd, nl, nr = [jnp.where(x, 1, 0) for x in (up, down, left, right)]
    pl.semaphore_wait(barrier, (1 + nu + nd) * (1 + nl + nr) - 1)

    def raw_send(s):
        if s == 0:
            return pltpu.make_async_remote_copy(img.at[:, pl.ds(0, 1)], raw.at[last, :, pl.ds(1, 1)],
                                                rh_send.at[0], rh_recv.at[0], device_id=dev(-1, 0), device_id_type=pl.DeviceIdType.MESH)
        return pltpu.make_async_remote_copy(img.at[:, pl.ds(2 * last - 1, 1)], raw.at[0, :, pl.ds(0, 1)],
                                            rh_send.at[1], rh_recv.at[1], device_id=dev(1, 0), device_id_type=pl.DeviceIdType.MESH)

    for there, s in zip((up, down), range(2)):
        @pl.when(there)
        def _(s=s):
            raw_send(s).start()

    def zero(ref):
        ref[...] = jnp.zeros(ref.shape, ref.dtype)

    def wide(ref, h):
        u = ref.shape[1] - 2
        return dict(ref=ref, h=h, hl=(0, 1), first=(1, 0), last=(u, 1), hr=(u + 1, 0), real=pl.ds(1, u))

    def flat(ref, h):
        w = ref.shape[1] - 2
        return dict(ref=ref, h=h, hl=(0,), first=(1,), last=(w,), hr=(w + 1,), real=pl.ds(1, w))

    bufs = [wide(y1, y1.shape[0] - 2), wide(z1, z1.shape[0] - 2), flat(y2, y2.shape[0] - 2), wide(z2, z2.shape[0] - 2),
            flat(y3, y3.shape[0] - 2)]

    for b in bufs:
        ref, h = b['ref'], b['h']

        @pl.when(jnp.logical_not(up))
        def _(ref=ref):
            zero(ref.at[0])

        @pl.when(jnp.logical_not(down))
        def _(ref=ref, h=h):
            zero(ref.at[h + 1])

        @pl.when(jnp.logical_not(left))
        def _(ref=ref, b=b, h=h):
            for r in range(h + 2):
                zero(ref.at[(r,) + b['hl']])

        @pl.when(jnp.logical_not(right))
        def _(ref=ref, b=b, h=h):
            for r in range(h + 2):
                zero(ref.at[(r,) + b['hr']])

    @pl.when(jnp.logical_not(up))
    def _():
        for n in range(nimg):
            zero(raw.at[0, n, 0])

    @pl.when(jnp.logical_not(down))
    def _():
        for n in range(nimg):
            zero(raw.at[last, n, 1])

    xu = xt.shape[1] - 2

    @pl.when(jnp.logical_not(left))
    def _():
        for k in range(last + 1):
            zero(xt.at[k, 0, 3])

    @pl.when(jnp.logical_not(right))
    def _():
        for k in range(last + 1):
            zero(xt.at[k, xu + 1, 0])

    def row_copy(i, s):
        b = bufs[i]
        ref, h = b['ref'], b['h']
        src, dst, dr = (1, h + 1, -1) if s == 0 else (h, 0, 1)
        return pltpu.make_async_remote_copy(ref.at[src, b['real']], ref.at[dst, b['real']], row_send.at[i, s], row_recv.at[i, s],
                                            device_id=dev(dr, 0), device_id_type=pl.DeviceIdType.MESH)

    def corner_copy(i, s):
        b = bufs[i]
        ref, h = b['ref'], b['h']
        dr, dc = near[4 + s][1:]
        src = (1 if dr < 0 else h,) + (b['first'] if dc < 0 else b['last'])
        dst = (h + 1 if dr < 0 else 0,) + (b['hr'] if dc < 0 else b['hl'])
        return pltpu.make_async_remote_copy(ref.at[src], ref.at[dst], cor_send.at[i, s], cor_recv.at[i, s],
                                            device_id=dev(dr, dc), device_id_type=pl.DeviceIdType.MESH)

    def col_copy(i, r, s):
        b = bufs[i]
        ref = b['ref']
        src, dst, dc = (b['first'], b['hr'], -1) if s == 0 else (b['last'], b['hl'], 1)
        return pltpu.make_async_remote_copy(ref.at[(r + 1,) + src], ref.at[(r + 1,) + dst], col_send.at[i, s], col_recv.at[i, r, s],
                                            device_id=dev(0, dc), device_id_type=pl.DeviceIdType.MESH)

    sides = ((left, 0), (right, 1))
    from_sides = ((right, 0), (left, 1))

    def each(cases, act):
        for there, s in cases:
            @pl.when(there)
            def _(s=s):
                act(s)

    def send_cols(i, r):
        each(sides, lambda s: col_copy(i, r, s).start())

    def wait_cols(i, r):
        each(from_sides, lambda s: col_copy(i, r, s).wait_recv())

    ends = list(zip((up, down), range(2)))
    from_ends = list(zip((down, up), range(2)))
    corners = [(x[0], s) for s, x in enumerate(near[4:])]
    from_corners = [(x[0], s) for s, x in enumerate(near[:3:-1])]

    def send_rows(i):
        each(ends, lambda s: row_copy(i, s).start())
        each(corners, lambda s: corner_copy(i, s).start())

    def wait_rows(i):
        each(from_ends, lambda s: row_copy(i, s).wait_recv())
        each(from_corners, lambda s: corner_copy(i, s).wait_recv())

    def xcol_copy(k, s):
        src, dst, dc = ((1, 0), (xu + 1, 0), -1) if s == 0 else ((xu, 3), (0, 3), 1)
        return pltpu.make_async_remote_copy(xt.at[(k,) + src], xt.at[(k,) + dst], xc_send.at[s], xc_recv.at[k, s],
                                            device_id=dev(0, dc), device_id_type=pl.DeviceIdType.MESH)

    def send_xcols(k):
        each(sides, lambda s: xcol_copy(k, s).start())

    def wait_xcols(k):
        each(from_sides, lambda s: xcol_copy(k, s).wait_recv())

    for i in (0, 1, 6, 7):
        wcopies[i].wait()
    zb = jnp.zeros((64, LANES), BF)
    for dk in range(2):
        for dc in range(3):
            for cpar in range(2):
                for rpar in range(2):
                    r0 = (dk * 3 + dc) * TILE + (cpar * 2 + rpar) * 64
                    for j in range(2):
                        q = 2 * (dc - j) + cpar
                        wp1[pl.ds(r0, 64), pl.ds(j * LANES, LANES)] = vwd1[2 * dk + rpar, q] if 0 <= q < 4 else zb
    zc = jnp.zeros((LANES, LANES), BF)
    for p in range(3):
        for s in range(4):
            for j in range(2):
                q = s - j
                wp2[pl.ds((p * 4 + s) * LANES, LANES), pl.ds(j * LANES, LANES)] = vwc1[p, q] if 0 <= q < 3 else zc

    eye = (lax.broadcasted_iota(jnp.int32, (LANES, LANES), 0) == lax.broadcasted_iota(jnp.int32, (LANES, LANES), 1)).astype(F32).astype(BF)

    def transpose_in(k, st):
        for s in range(nimg // 2):
            rhs = raw[k, pl.ds(2 * s, 2)].reshape(TILE, LANES)
            t = lax.dot_general(eye, rhs, BY_LAST, preferred_element_type=F32)
            st[pl.ds(2 * s * PITCH, LANES), :] = t[:, :LANES]
            st[pl.ds((2 * s + 1) * PITCH, LANES), :] = t[:, LANES:]

    def transpose_out(k, st):
        for c in range(4 * xu):
            xt[k, 1 + c // 4, c % 4] = st[pl.ds(c, nimg, stride=PITCH), :].astype(BF)

    def middle_out(t):
        h = (t + 1) // 2
        return mid + h * (1 - 2 * (t % 2))

    def take_three(it, carry):
        ks = [middle_out(3 * it + d) for d in range(3)]

        @pl.when(it < 3)
        def _():
            for d in range(3):
                raw_copy(middle_out(3 * it + 6 + d)).start()

        @pl.when(it == 3)
        def _():
            first_copy.start()
            last_copy.start()
        sts = [st0, st1, st2]
        for k in ks:
            raw_copy(k).wait()
        for k, st in zip(ks, sts):
            transpose_in(k, st)
        for k, st in zip(ks, sts):
            transpose_out(k, st)
        for k in ks:
            send_xcols(k)
        return carry

    lax.fori_loop(0, (last - 1) // 3, take_three, 0)
    for i in range(2, 6):
        wcopies[i].start()
        wcopies[i + 6].start()

    def take_edges():
        first_copy.wait()
        last_copy.wait()

        each(from_ends, lambda s: raw_send(s).wait_recv())
        transpose_in(0, st0)
        transpose_in(last, st1)
        transpose_out(0, st0)
        transpose_out(last, st1)
        send_xcols(0)
        send_xcols(last)

    def finish(acc, bias):
        return jnp.maximum(acc + bias, 0.0).astype(BF)

    def put_pairs(ref, i, v):
        for j in range(2):
            ref[i + 1, pl.ds(1, pairs), j] = v[:, j * LANES:(j + 1) * LANES].reshape(pairs, nimg, LANES)

    def rows_of(ref, idx, w):
        v = ref[idx]
        return v.reshape(w * nimg, v.shape[-1])

    def wait_pair(i, a, h):
        wait_cols(i, a)
        wait_cols(i, h - 1 - a)

    def step_of(t, n, p):
        up_now = (t + n - p) // n
        return (1 - up_now) * (n - 1 - t) + up_now * (t - p)

    def wait_conv(i, t, a, h, p):
        n = h // 2
        seen = n - 1 - p if p else n

        if p:
            @pl.when(t == 0)
            def _():
                wait_pair(i, n - 1, h)

            @pl.when(t < p)
            def _():
                wait_pair(i, a - 1, h)

        @pl.when(t == p)
        def _():
            wait_pair(i, 0, h)
            wait_rows(i)

        @pl.when((t >= p) & (a + 1 < seen))
        def _():
            wait_pair(i, a + 1, h)

    def wait_down(i, a, h):
        @pl.when(a == 0)
        def _():
            wait_pair(i, 0, 2 * h)
            wait_rows(i)
        wait_pair(i, 2 * a + 1, 2 * h)

        @pl.when(a < h // 2 - 1)
        def _():
            wait_pair(i, 2 * a + 2, 2 * h)

    def send(i, t, a, h, e):
        send_cols(i, a)
        send_cols(i, h - 1 - a)

        @pl.when(t == e)
        def _():
            send_rows(i)

    pairs = y1.shape[1] - 2
    bias1 = jnp.concatenate([vb1[...], vb1[...]], axis=-1)
    h1 = y1.shape[0] - 2

    e1 = 4

    def wait_images(t, a):
        @pl.when(t == 0)
        def _():
            wait_xcols(mid)

        @pl.when(t < e1)
        def _():
            wait_xcols(a)
            wait_xcols(last - a)

        @pl.when(t == e1)
        def _():
            wait_xcols(0)
            wait_xcols(last)

        @pl.when((t >= e1) & (a + 1 < h1 // 2 - e1))
        def _():
            wait_xcols(a + 1)
            wait_xcols(last - 1 - a)

    def down1(a):
        for i in (a, h1 - 1 - a):
            parts = []
            for dk in range(2):
                for p in range(3, 9):
                    parts.append(rows_of(xt, (i + dk, pl.ds(p // 4, pairs), p % 4), pairs))
            acc = jnp.dot(jnp.concatenate(parts, axis=-1), wp1[...], preferred_element_type=F32)
            v = finish(acc, bias1)
            put_pairs(y1, i, v)

    def two_steps(wait, step, i, h, p, before=lambda t2: None):
        def body(t2, carry):
            before(t2)
            ts = [2 * t2, 2 * t2 + 1]
            steps = [step_of(t, h // 2, p) for t in ts]
            for t, a in zip(ts, steps):
                wait(t, a)
            for a in steps:
                step(a)
            for t, a in zip(ts, steps):
                send(i, t, a, h, p)
            return carry
        lax.fori_loop(0, h // 4, body, 0)

    def first_then_rest(wait, step, i, h):
        for steps in ([0], list(range(1, h // 2))):
            for a in steps:
                wait(a, a)
            for a in steps:
                step(a)
            for a in steps:
                send(i, a, a, h, 0)

    def edges_at(t2):
        @pl.when(t2 == e1 // 2 - 1)
        def _():
            take_edges()

    two_steps(wait_images, down1, 0, h1, e1, edges_at)

    bias2 = jnp.concatenate([vb2[...], vb2[...]], axis=-1)

    def conv1(a):
        for i in (a, h1 - 1 - a):
            parts = []
            for p in range(3):
                for s in range(1, 5):
                    parts.append(rows_of(y1, (i + p, pl.ds(s // 2, pairs), s % 2), pairs))
            acc = jnp.dot(jnp.concatenate(parts, axis=-1), wp2[...], preferred_element_type=F32)
            v = finish(acc, bias2)
            put_pairs(z1, i, v)

    two_steps(lambda t, a: wait_conv(0, t, a, h1, 2), conv1, 1, h1, 2)

    ch3 = out.shape[-1]
    h2 = y2.shape[0] - 2
    w2 = y2.shape[1] - 2
    for i in (2, 8):
        wcopies[i].wait()

    def down2(a):
        for i in (a, h2 - 1 - a):
            parts = []
            for p in range(4):
                for s in range(1, 5):
                    parts.append(rows_of(z1, (2 * i + p, pl.ds(s // 2, w2), s % 2), w2))
            acc = jnp.dot(jnp.concatenate(parts, axis=-1), vwd2[...].reshape(16 * LANES, TILE), preferred_element_type=F32)
            y2[i + 1, pl.ds(1, w2)] = finish(acc, vb3[...]).reshape(w2, nimg, TILE)

    first_then_rest(lambda t, a: wait_down(1, a, h2), down2, 2, h2)
    for i in (3, 9, 5):
        wcopies[i].wait()
    wp6[...] = jnp.zeros(wp6.shape, BF)
    for p in range(3):
        for q in range(3):
            wp6[p * 3 + q, pl.ds(0, ch3), :] = vwc3[p, q]

    def conv2(a):
        for i in (a, h2 - 1 - a):
            parts = []
            for p in range(3):
                for q in range(3):
                    parts.append(rows_of(y2, (i + p, pl.ds(q, w2)), w2))
            acc = jnp.dot(jnp.concatenate(parts, axis=-1), vwc2[...].reshape(9 * TILE, TILE), preferred_element_type=F32)
            v = finish(acc, vb4[...]).reshape(w2 // 2, 2, nimg, TILE)
            z2[i + 1, pl.ds(1, w2 // 2), 0] = v[:, 0]
            z2[i + 1, pl.ds(1, w2 // 2), 1] = v[:, 1]

    first_then_rest(lambda t, a: wait_conv(2, t, a, h2, 0), conv2, 3, h2)

    h3 = y3.shape[0] - 2
    w3 = y3.shape[1] - 2
    for i in (4, 10, 11):
        wcopies[i].wait()

    def down3(t, carry):
        a = t
        wait_down(3, a, h3)
        ii = (a, h3 - 1 - a)
        acc = None
        for p in range(4):
            for s in range(1, 5):
                lhs = jnp.concatenate([rows_of(z2, (2 * i + p, pl.ds(s // 2, w3), s % 2), w3) for i in ii], axis=0)
                d = lax.dot_general(lhs, vwd3[p, s - 1], BY_LAST, preferred_element_type=F32)
                acc = d if acc is None else acc + d
        v = finish(acc, vb5[...])
        v = jnp.concatenate([v, jnp.zeros((v.shape[0], y3.shape[-1] - ch3), BF)], axis=-1)
        for n, i in enumerate(ii):
            y3[i + 1, pl.ds(1, w3)] = v[n * w3 * nimg:(n + 1) * w3 * nimg].reshape(w3, nimg, y3.shape[-1])
        send(4, t, a, h3, 0)
        return carry

    lax.fori_loop(0, h3 // 2, down3, 0)

    inner = [(i, 1, w3 - 2) for i in range(1, h3 - 1)]
    border = [(0, 0, w3), (h3 - 1, 0, w3)] + [(i, c, 1) for i in range(1, h3 - 1) for c in (0, w3 - 1)]

    def conv3(strips):
        parts = []
        for p in range(3):
            for q in range(3):
                parts.append(jnp.concatenate([rows_of(y3, (i + p, pl.ds(c + q, w)), w) for i, c, w in strips], axis=0))
        acc = jnp.dot(jnp.concatenate(parts, axis=-1), wp6[...].reshape(9 * wp6.shape[1], ch3), preferred_element_type=F32)
        v = finish(acc, vb6[...])
        at = 0
        for i, c, w in strips:
            out[i, pl.ds(c, w)] = v[at:at + w * nimg].reshape(w, nimg, ch3)
            at += w * nimg

    conv3(inner)
    for r in range(h3):
        wait_cols(4, r)
    wait_rows(4)
    conv3(border)

    each(ends, lambda s: raw_send(s).wait_send())

    def drain_cols(ref, rows, at, sem):
        whole = ref.at[(rows,) + at]
        pltpu.make_async_remote_copy(whole, whole, sem, sem, device_id=dev(0, 0), device_id_type=pl.DeviceIdType.MESH).wait_send()

    each(sides, lambda s: drain_cols(xt, pl.ds(0, last + 1), (1, 0), xc_send.at[s]))
    for i, b in enumerate(bufs):
        each(ends, lambda s: row_copy(i, s).wait_send())
        each(corners, lambda s: corner_copy(i, s).wait_send())
        each(sides, lambda s: drain_cols(b['ref'], pl.ds(1, b['h']), b['first'], col_send.at[i, s]))


def solution(mesh):
    dims = (mesh.shape['row'], mesh.shape['col'])

    def local_encoder(images, w_down1, b_down1, w_conv1, b_conv1, w_down2, b_down2, w_conv2, b_conv2, w_down3, b_down3, w_conv3, b_conv3):
        n, h, w, c = images.shape
        img = jnp.transpose(images, (0, 1, 3, 2))
        wd3 = jnp.transpose(w_down3, (0, 1, 3, 2))
        c1, c2, c3 = w_conv1.shape[-1], w_conv2.shape[-1], w_conv3.shape[-1]
        c3p = pl.cdiv(c3, LANES) * LANES
        hbm = pl.BlockSpec(memory_space=pl.ANY)
        dma = pltpu.SemaphoreType.DMA
        hh, hq, he = h // 2, h // 4, h // 8
        wq, we = w // 4, w // 8
        kk = hh + 1
        scratch = [
            pltpu.VMEM((kk, n, 2, c, w), BF),
            pltpu.VMEM((kk, wq + 2, 4, n, 2 * c), BF),
            pltpu.VMEM((hh + 2, wq + 2, 2, n, c1), BF),
            pltpu.VMEM((hh + 2, wq + 2, 2, n, c1), BF),
            pltpu.VMEM((hq + 2, wq + 2, n, c2), BF),
            pltpu.VMEM((hq + 2, we + 2, 2, n, c2), BF),
            pltpu.VMEM((he + 2, we + 2, n, c3p), BF),
        ] + [pltpu.VMEM((n * PITCH, LANES), F32)] * 3 + [
            pltpu.VMEM(x.shape, BF) for x in (w_down1, w_conv1, w_down2, w_conv2, wd3, w_conv3)
        ] + [
            pltpu.VMEM((6 * TILE, TILE), BF),
            pltpu.VMEM((6 * TILE, TILE), BF),
            pltpu.VMEM((9, c3p, c3), BF),
        ] + [pltpu.VMEM((1, k), F32) for k in (c1, c1, c2, c2, c3, c3)] + [
            dma(d) for d in ((kk,), (12,), (2,), (2,), (2,), (kk, 2), (5, 2), (5, 2), (5, 4), (5, 4), (5, 2), (5, hh, 2))
        ]
        feats = pl.pallas_call(
            functools.partial(_encoder_kernel, dims),
            out_shape=jax.ShapeDtypeStruct((he, we, n, c3), BF),
            in_specs=[hbm] * 13,
            out_specs=pl.BlockSpec(memory_space=pltpu.VMEM),
            scratch_shapes=scratch,
            compiler_params=pltpu.CompilerParams(collective_id=0, has_side_effects=True, vmem_limit_bytes=62 * 1024 * 1024),
        )(img, w_down1, b_down1, w_conv1, b_conv1, w_down2, b_down2, w_conv2, b_conv2, wd3, b_down3, w_conv3, b_conv3)
        return jnp.transpose(feats, (2, 0, 1, 3))

    tile_spec = P('batch', 'row', 'col', None)
    return jax.shard_map(local_encoder, mesh=mesh, in_specs=(tile_spec,) + (P(),) * 12, out_specs=tile_spec, check_vma=False)
```

```python
import functools

import jax
import jax.numpy as jnp
from jax import lax
from jax.experimental import pallas as pl
from jax.experimental.pallas import tpu as pltpu
from jax.sharding import PartitionSpec as P

BY_LAST = (((1,), (1,)), ((), ()))
BF = jnp.bfloat16
F32 = jnp.float32
LANES = 128
TILE = 2 * LANES
PITCH = 129


def _encoder_kernel(dims, img, wd1, bd1, wc1, bc1, wd2, bd2, wc2, bc2, wd3, bd3, wc3, bc3, out,
                    raw, xt, y1, z1, y2, z2, y3, st0, st1, st2,
                    vwd1, vwc1, vwd2, vwc2, vwd3, vwc3, wp1, wp2, wp6,
                    vb1, vb2, vb3, vb4, vb5, vb6,
                    raw_sem, w_sem, rh_send, rh_recv, xc_send, xc_recv,
                    row_send, row_recv, cor_send, cor_recv, col_send, col_recv):
    row_len, col_len = dims
    nimg = img.shape[0]
    my_row = lax.axis_index('row')
    my_col = lax.axis_index('col')
    up, down = my_row > 0, my_row < row_len - 1
    left, right = my_col > 0, my_col < col_len - 1

    def both(a, b):
        return jnp.logical_and(a, b)

    near = [(up, -1, 0), (down, 1, 0), (left, 0, -1), (right, 0, 1)]
    near += [(both(v[0], g[0]), v[1], g[2]) for v in near[:2] for g in near[2:]]

    def dev(dr, dc):
        return {'row': my_row + dr, 'col': my_col + dc}

    def raw_copy(k):
        return pltpu.make_async_copy(img.at[:, pl.ds(2 * k - 1, 2)], raw.at[k], raw_sem.at[k])

    last = raw.shape[0] - 1
    mid = last // 2
    first_copy = pltpu.make_async_copy(img.at[:, pl.ds(0, 1)], raw.at[0, :, pl.ds(1, 1)], raw_sem.at[0])
    last_copy = pltpu.make_async_copy(img.at[:, pl.ds(2 * last - 1, 1)], raw.at[last, :, pl.ds(0, 1)], raw_sem.at[last])
    order = []
    for t in range(last - 1):
        h = (t + 1) // 2
        order.append(mid - h if t % 2 else mid + h)
    weights = [(wd1, vwd1), (wc1, vwc1), (wd2, vwd2), (wc2, vwc2), (wd3, vwd3), (wc3, vwc3),
               *((x, v.at[0]) for x, v in zip((bd1, bc1, bd2, bc2, bd3, bc3), (vb1, vb2, vb3, vb4, vb5, vb6)))]
    wcopies = [pltpu.make_async_copy(s, d, w_sem.at[i]) for i, (s, d) in enumerate(weights)]
    for i in (0, 6, 1, 7):
        wcopies[i].start()
    for k in order[:6]:
        raw_copy(k).start()

    barrier = pltpu.get_barrier_semaphore()
    for there, dr, dc in near:
        @pl.when(there)
        def _(dr=dr, dc=dc):
            pl.semaphore_signal(barrier, inc=1, device_id=dev(dr, dc), device_id_type=pl.DeviceIdType.MESH)
    nu, nd, nl, nr = [jnp.where(x, 1, 0) for x in (up, down, left, right)]
    pl.semaphore_wait(barrier, (1 + nu + nd) * (1 + nl + nr) - 1)

    def raw_send(s):
        if s == 0:
            return pltpu.make_async_remote_copy(img.at[:, pl.ds(0, 1)], raw.at[last, :, pl.ds(1, 1)],
                                                rh_send.at[0], rh_recv.at[0], device_id=dev(-1, 0), device_id_type=pl.DeviceIdType.MESH)
        return pltpu.make_async_remote_copy(img.at[:, pl.ds(2 * last - 1, 1)], raw.at[0, :, pl.ds(0, 1)],
                                            rh_send.at[1], rh_recv.at[1], device_id=dev(1, 0), device_id_type=pl.DeviceIdType.MESH)

    for there, s in zip((up, down), range(2)):
        @pl.when(there)
        def _(s=s):
            raw_send(s).start()

    def zero(ref):
        ref[...] = jnp.zeros(ref.shape, ref.dtype)

    def wide(ref, h):
        u = ref.shape[1] - 2
        return dict(ref=ref, h=h, hl=(0, 1), first=(1, 0), last=(u, 1), hr=(u + 1, 0), real=pl.ds(1, u))

    def flat(ref, h):
        w = ref.shape[1] - 2
        return dict(ref=ref, h=h, hl=(0,), first=(1,), last=(w,), hr=(w + 1,), real=pl.ds(1, w))

    bufs = [wide(y1, y1.shape[0] - 2), wide(z1, z1.shape[0] - 2), flat(y2, y2.shape[0] - 2), wide(z2, z2.shape[0] - 2),
            flat(y3, y3.shape[0] - 2)]

    for b in bufs:
        ref, h = b['ref'], b['h']

        @pl.when(jnp.logical_not(up))
        def _(ref=ref):
            zero(ref.at[0])

        @pl.when(jnp.logical_not(down))
        def _(ref=ref, h=h):
            zero(ref.at[h + 1])

        @pl.when(jnp.logical_not(left))
        def _(ref=ref, b=b, h=h):
            for r in range(h + 2):
                zero(ref.at[(r,) + b['hl']])

        @pl.when(jnp.logical_not(right))
        def _(ref=ref, b=b, h=h):
            for r in range(h + 2):
                zero(ref.at[(r,) + b['hr']])

    @pl.when(jnp.logical_not(up))
    def _():
        for n in range(nimg):
            zero(raw.at[0, n, 0])

    @pl.when(jnp.logical_not(down))
    def _():
        for n in range(nimg):
            zero(raw.at[last, n, 1])

    xu = xt.shape[1] - 2

    @pl.when(jnp.logical_not(left))
    def _():
        for k in range(last + 1):
            zero(xt.at[k, 0, 3])

    @pl.when(jnp.logical_not(right))
    def _():
        for k in range(last + 1):
            zero(xt.at[k, xu + 1, 0])

    def row_copy(i, s):
        b = bufs[i]
        ref, h = b['ref'], b['h']
        src, dst, dr = (1, h + 1, -1) if s == 0 else (h, 0, 1)
        return pltpu.make_async_remote_copy(ref.at[src, b['real']], ref.at[dst, b['real']], row_send.at[i, s], row_recv.at[i, s],
                                            device_id=dev(dr, 0), device_id_type=pl.DeviceIdType.MESH)

    def corner_copy(i, s):
        b = bufs[i]
        ref, h = b['ref'], b['h']
        dr, dc = near[4 + s][1:]
        src = (1 if dr < 0 else h,) + (b['first'] if dc < 0 else b['last'])
        dst = (h + 1 if dr < 0 else 0,) + (b['hr'] if dc < 0 else b['hl'])
        return pltpu.make_async_remote_copy(ref.at[src], ref.at[dst], cor_send.at[i, s], cor_recv.at[i, s],
                                            device_id=dev(dr, dc), device_id_type=pl.DeviceIdType.MESH)

    def col_copy(i, r, s):
        b = bufs[i]
        ref = b['ref']
        src, dst, dc = (b['first'], b['hr'], -1) if s == 0 else (b['last'], b['hl'], 1)
        return pltpu.make_async_remote_copy(ref.at[(r + 1,) + src], ref.at[(r + 1,) + dst], col_send.at[i, s], col_recv.at[i, r, s],
                                            device_id=dev(0, dc), device_id_type=pl.DeviceIdType.MESH)

    sides = ((left, 0), (right, 1))
    from_sides = ((right, 0), (left, 1))

    def each(cases, act):
        for there, s in cases:
            @pl.when(there)
            def _(s=s):
                act(s)

    ends = list(zip((up, down), range(2)))
    from_ends = list(zip((down, up), range(2)))
    corners = [(x[0], s) for s, x in enumerate(near[4:])]
    from_corners = [(x[0], s) for s, x in enumerate(near[:3:-1])]

    def send_rows(i):
        each(ends, lambda s: row_copy(i, s).start())
        each(corners, lambda s: corner_copy(i, s).start())

    def wait_rows(i):
        each(from_ends, lambda s: row_copy(i, s).wait_recv())
        each(from_corners, lambda s: corner_copy(i, s).wait_recv())

    def xcol_copy(k, s):
        src, dst, dc = ((1, 0), (xu + 1, 0), -1) if s == 0 else ((xu, 3), (0, 3), 1)
        return pltpu.make_async_remote_copy(xt.at[(k,) + src], xt.at[(k,) + dst], xc_send.at[s], xc_recv.at[k, s],
                                            device_id=dev(0, dc), device_id_type=pl.DeviceIdType.MESH)

    def send_xcols(ks):
        each(sides, lambda s: [xcol_copy(k, s).start() for k in ks])

    def wait_xcols(*ks):
        each(from_sides, lambda s: [xcol_copy(k, s).wait_recv() for k in ks])

    for i in (0, 1, 6, 7):
        wcopies[i].wait()

    def loop(count, act):
        def body(i, carry):
            act(i)
            return carry
        lax.fori_loop(0, count, body, 0)

    def zero_block(ref):
        def act(i):
            zero(ref.at[i])
        return act

    def fill1(i):
        dk, dc, cpar, rpar = i // 8, i // 4 % 2, i // 2 % 2, i % 2
        for j in range(2):
            wp1[(dk * 3 + dc + j) * 4 + cpar * 2 + rpar, :, pl.ds(j * LANES, LANES)] = vwd1[2 * dk + rpar, 2 * dc + cpar]

    def fill2(i):
        for j in range(2):
            wp2[i // 3 * 4 + i % 3 + j, :, pl.ds(j * LANES, LANES)] = vwc1[i // 3, i % 3]

    loop(wp1.shape[0], zero_block(wp1))
    loop(wp2.shape[0], zero_block(wp2))
    loop(16, fill1)
    loop(9, fill2)

    eye = (lax.broadcasted_iota(jnp.int32, (LANES, LANES), 0) == lax.broadcasted_iota(jnp.int32, (LANES, LANES), 1)).astype(F32).astype(BF)

    def transpose_in(k, st):
        for s in range(nimg // 2):
            rhs = raw[k, pl.ds(2 * s, 2)].reshape(TILE, LANES)
            t = lax.dot_general(eye, rhs, BY_LAST, preferred_element_type=F32)
            st[pl.ds(2 * s * PITCH, LANES), :] = t[:, :LANES]
            st[pl.ds((2 * s + 1) * PITCH, LANES), :] = t[:, LANES:]

    def transpose_out(k, st):
        for c in range(4 * xu):
            xt[k, 1 + c // 4, c % 4] = st[pl.ds(c, nimg, stride=PITCH), :].astype(BF)

    def middle_out(t):
        h = (t + 1) // 2
        return mid + h * (1 - 2 * (t % 2))

    inner = (last - 1) // 3

    def take_three(it, carry):
        edge = it // inner
        ks = [edge * (last * min(d, 1)) + (1 - edge) * middle_out(3 * it + d) for d in range(3)]

        @pl.when(it < inner - 2)
        def _():
            for d in range(3):
                raw_copy(middle_out(3 * it + 6 + d)).start()

        @pl.when(it == inner - 2)
        def _():
            first_copy.start()
            last_copy.start()

        @pl.when(it < inner)
        def _():
            for k in ks:
                raw_copy(k).wait()

        @pl.when(it == inner)
        def _():
            first_copy.wait()
            last_copy.wait()
            each(from_ends, lambda s: raw_send(s).wait_recv())
        for k, st in zip(ks, (st0, st1, st2)):
            transpose_in(k, st)
        for k, st in zip(ks, (st0, st1, st2)):
            transpose_out(k, st)
        send_xcols(ks[:2])

        @pl.when(it < inner)
        def _():
            send_xcols(ks[2:])
        return carry

    def finish(acc, bias):
        return jnp.maximum(acc + bias, 0.0).astype(BF)

    def put_pairs(ref, i, v):
        for j in range(2):
            ref[i + 1, pl.ds(1, pairs), j] = v[:, j * LANES:(j + 1) * LANES].reshape(pairs, nimg, LANES)

    def rows_of(ref, idx, w):
        v = ref[idx]
        return v.reshape(w * nimg, v.shape[-1])

    def wait_pair(i, a, h):
        each(from_sides, lambda s: [col_copy(i, r, s).wait_recv() for r in (a, h - 1 - a)])

    def step_of(t, n, p):
        up_now = (t + n - p) // n
        return (1 - up_now) * (n - 1 - t) + up_now * (t - p)

    def wait_conv(i, t, a, h, p):
        n = h // 2
        seen = n - 1 - p if p else n

        if p:
            @pl.when(t == 0)
            def _():
                wait_pair(i, n - 1, h)

            @pl.when(t < p)
            def _():
                wait_pair(i, a - 1, h)

        @pl.when(t == p)
        def _():
            wait_pair(i, 0, h)
            wait_rows(i)

        @pl.when(jnp.logical_and(t >= p, a + 1 < seen))
        def _():
            wait_pair(i, a + 1, h)

    def wait_down(i, a, h):
        @pl.when(a == 0)
        def _():
            wait_pair(i, 0, 2 * h)
            wait_rows(i)
        wait_pair(i, 2 * a + 1, 2 * h)

        @pl.when(a < h // 2 - 1)
        def _():
            wait_pair(i, 2 * a + 2, 2 * h)

    def send(i, t, a, h, e):
        each(sides, lambda s: [col_copy(i, r, s).start() for r in (a, h - 1 - a)])

        @pl.when(t == e)
        def _():
            send_rows(i)

    pairs = y1.shape[1] - 2
    bias1 = jnp.concatenate([vb1[...], vb1[...]], axis=-1)
    h1 = y1.shape[0] - 2

    e1 = 4

    def down1(t, carry):
        a = step_of(t, h1 // 2, e1)

        @pl.when(t == 0)
        def _():
            wait_xcols(mid)

        @pl.when(t < e1)
        def _():
            wait_xcols(a, last - a)

        @pl.when(t == e1)
        def _():
            wait_xcols(0, last)

        @pl.when(jnp.logical_and(t >= e1, a + 1 < h1 // 2 - e1))
        def _():
            wait_xcols(a + 1, last - 1 - a)
        for i in (a, h1 - 1 - a):
            parts = []
            for dk in range(2):
                for p in range(3, 9):
                    parts.append(rows_of(xt, (i + dk, pl.ds(p // 4, pairs), p % 4), pairs))
            acc = jnp.dot(jnp.concatenate(parts, axis=-1), wp1[...].reshape(6 * TILE, TILE), preferred_element_type=F32)
            v = finish(acc, bias1)
            put_pairs(y1, i, v)
        send(0, t, a, h1, e1)
        return carry

    def phase(ph, carry):
        lax.fori_loop(inner * ph, inner + ph, take_three, 0)

        @pl.when(ph == 0)
        def _():
            for i in range(2, 6):
                wcopies[i].start()
                wcopies[i + 6].start()
        lax.fori_loop((e1 - 2) * ph, e1 - 2 + (h1 // 2 - e1 + 2) * ph, down1, 0)
        return carry

    lax.fori_loop(0, 2, phase, 0)

    bias2 = jnp.concatenate([vb2[...], vb2[...]], axis=-1)

    def conv1(t, carry):
        a = step_of(t, h1 // 2, 2)
        wait_conv(0, t, a, h1, 2)
        for i in (a, h1 - 1 - a):
            parts = []
            for p in range(3):
                for s in range(1, 5):
                    parts.append(rows_of(y1, (i + p, pl.ds(s // 2, pairs), s % 2), pairs))
            acc = jnp.dot(jnp.concatenate(parts, axis=-1), wp2[...].reshape(6 * TILE, TILE), preferred_element_type=F32)
            v = finish(acc, bias2)
            put_pairs(z1, i, v)
        send(1, t, a, h1, 2)
        return carry

    lax.fori_loop(0, h1 // 2, conv1, 0)

    ch3 = out.shape[-1]
    h2 = y2.shape[0] - 2
    w2 = y2.shape[1] - 2
    for i in (2, 8):
        wcopies[i].wait()

    def down2(t, carry):
        a = t
        wait_down(1, a, h2)
        for i in (a, h2 - 1 - a):
            parts = []
            for p in range(4):
                for s in range(1, 5):
                    parts.append(rows_of(z1, (2 * i + p, pl.ds(s // 2, w2), s % 2), w2))
            acc = jnp.dot(jnp.concatenate(parts, axis=-1), vwd2[...].reshape(16 * LANES, TILE), preferred_element_type=F32)
            y2[i + 1, pl.ds(1, w2)] = finish(acc, vb3[...]).reshape(w2, nimg, TILE)
        send(2, t, a, h2, 0)
        return carry

    lax.fori_loop(0, h2 // 2, down2, 0)
    for i in (3, 9, 5):
        wcopies[i].wait()

    def fill6(i):
        wp6[i, pl.ds(0, ch3), :] = vwc3[i // 3, i % 3]
        wp6[i, pl.ds(ch3, wp6.shape[1] - ch3), :] = jnp.zeros((wp6.shape[1] - ch3, ch3), BF)

    loop(9, fill6)

    def conv2(t, carry):
        a = t
        wait_conv(2, t, a, h2, 0)
        for i in (a, h2 - 1 - a):
            parts = []
            for p in range(3):
                for q in range(3):
                    parts.append(rows_of(y2, (i + p, pl.ds(q, w2)), w2))
            acc = jnp.dot(jnp.concatenate(parts, axis=-1), vwc2[...].reshape(9 * TILE, TILE), preferred_element_type=F32)
            v = finish(acc, vb4[...]).reshape(w2 // 2, 2, nimg, TILE)
            z2[i + 1, pl.ds(1, w2 // 2), 0] = v[:, 0]
            z2[i + 1, pl.ds(1, w2 // 2), 1] = v[:, 1]
        send(3, t, a, h2, 0)
        return carry

    lax.fori_loop(0, h2 // 2, conv2, 0)

    h3 = y3.shape[0] - 2
    w3 = y3.shape[1] - 2
    for i in (4, 10, 11):
        wcopies[i].wait()

    def down3(t, carry):
        a = t
        wait_down(3, a, h3)
        ii = (a, h3 - 1 - a)
        parts, wts = [], []
        for p in range(4):
            for s in range(1, 5):
                parts.append(jnp.concatenate([rows_of(z2, (2 * i + p, pl.ds(s // 2, w3), s % 2), w3) for i in ii], axis=0))
                wts.append(vwd3[p, s - 1])
        acc = lax.dot_general(jnp.concatenate(parts, axis=-1), jnp.concatenate(wts, axis=-1), BY_LAST, preferred_element_type=F32)
        v = finish(acc, vb5[...])
        v = jnp.concatenate([v, jnp.zeros((v.shape[0], y3.shape[-1] - ch3), BF)], axis=-1)
        for n, i in enumerate(ii):
            y3[i + 1, pl.ds(1, w3)] = v[n * w3 * nimg:(n + 1) * w3 * nimg].reshape(w3, nimg, y3.shape[-1])
        send(4, t, a, h3, 0)
        return carry

    lax.fori_loop(0, h3 // 2, down3, 0)

    def conv3(t, carry):
        @pl.when(t == 1)
        def _():
            for r in range(h3 // 2):
                wait_pair(4, r, h3)
            wait_rows(4)
        top, bottom, lo, hi = 1 - t, h3 - 2 + t, 1 - t, w3 - 2 + t
        strips = [(i, 1, w3 - 2) for i in (top, bottom)] + [(i, c, 1) for i in (top, bottom, *range(1, h3 - 1)) for c in (lo, hi)]
        parts = []
        for p in range(3):
            for q in range(3):
                parts.append(jnp.concatenate([rows_of(y3, (i + p, pl.ds(c + q, w)), w) for i, c, w in strips], axis=0))
        acc = jnp.dot(jnp.concatenate(parts, axis=-1), wp6[...].reshape(9 * wp6.shape[1], ch3), preferred_element_type=F32)
        v = finish(acc, vb6[...])
        at = 0
        for i, c, w in strips:
            out[i, pl.ds(c, w)] = v[at:at + w * nimg].reshape(w, nimg, ch3)
            at += w * nimg
        return carry

    lax.fori_loop(0, 2, conv3, 0)

    each(ends, lambda s: raw_send(s).wait_send())

    def drain_cols(ref, rows, at, sem):
        whole = ref.at[(rows,) + at]
        pltpu.make_async_remote_copy(whole, whole, sem, sem, device_id=dev(0, 0), device_id_type=pl.DeviceIdType.MESH).wait_send()

    each(sides, lambda s: drain_cols(xt, pl.ds(0, last + 1), (1, 0), xc_send.at[s]))
    for i, b in enumerate(bufs):
        each(ends, lambda s: row_copy(i, s).wait_send())
        each(corners, lambda s: corner_copy(i, s).wait_send())
        each(sides, lambda s: drain_cols(b['ref'], pl.ds(1, b['h']), b['first'], col_send.at[i, s]))


def solution(mesh):
    dims = (mesh.shape['row'], mesh.shape['col'])

    def local_encoder(images, w_down1, b_down1, w_conv1, b_conv1, w_down2, b_down2, w_conv2, b_conv2, w_down3, b_down3, w_conv3, b_conv3):
        n, h, w, c = images.shape
        img = jnp.transpose(images, (0, 1, 3, 2))
        wd3 = jnp.transpose(w_down3, (0, 1, 3, 2))
        c1, c2, c3 = w_conv1.shape[-1], w_conv2.shape[-1], w_conv3.shape[-1]
        c3p = pl.cdiv(c3, LANES) * LANES
        hbm = pl.BlockSpec(memory_space=pl.ANY)
        dma = pltpu.SemaphoreType.DMA
        hh, hq, he = h // 2, h // 4, h // 8
        wq, we = w // 4, w // 8
        kk = hh + 1
        scratch = [
            pltpu.VMEM((kk, n, 2, c, w), BF),
            pltpu.VMEM((kk, wq + 2, 4, n, 2 * c), BF),
            pltpu.VMEM((hh + 2, wq + 2, 2, n, c1), BF),
            pltpu.VMEM((hh + 2, wq + 2, 2, n, c1), BF),
            pltpu.VMEM((hq + 2, wq + 2, n, c2), BF),
            pltpu.VMEM((hq + 2, we + 2, 2, n, c2), BF),
            pltpu.VMEM((he + 2, we + 2, n, c3p), BF),
        ] + [pltpu.VMEM((n * PITCH, LANES), F32)] * 3 + [
            pltpu.VMEM(x.shape, BF) for x in (w_down1, w_conv1, w_down2, w_conv2, wd3, w_conv3)
        ] + [
            pltpu.VMEM((24, c, TILE), BF),
            pltpu.VMEM((12, c1, TILE), BF),
            pltpu.VMEM((9, c3p, c3), BF),
        ] + [pltpu.VMEM((1, k), F32) for k in (c1, c1, c2, c2, c3, c3)] + [
            dma(d) for d in ((kk,), (12,), (2,), (2,), (2,), (kk, 2), (5, 2), (5, 2), (5, 4), (5, 4), (5, 2), (5, hh, 2))
        ]
        feats = pl.pallas_call(
            functools.partial(_encoder_kernel, dims),
            out_shape=jax.ShapeDtypeStruct((he, we, n, c3), BF),
            in_specs=[hbm] * 13,
            out_specs=pl.BlockSpec(memory_space=pltpu.VMEM),
            scratch_shapes=scratch,
            compiler_params=pltpu.CompilerParams(collective_id=0, has_side_effects=True, vmem_limit_bytes=62 * 1024 * 1024),
        )(img, w_down1, b_down1, w_conv1, b_conv1, w_down2, b_down2, w_conv2, b_conv2, wd3, b_down3, w_conv3, b_conv3)
        return jnp.transpose(feats, (2, 0, 1, 3))

    tile_spec = P('batch', 'row', 'col', None)
    return jax.shard_map(local_encoder, mesh=mesh, in_specs=(tile_spec,) + (P(),) * 12, out_specs=tile_spec, check_vma=False)
```

```python
import functools

import jax
import jax.numpy as jnp
from jax import lax
from jax.experimental import pallas as pl
from jax.experimental.pallas import tpu as pltpu
from jax.sharding import PartitionSpec as P

BY_LAST = (((1,), (1,)), ((), ()))
BF = jnp.bfloat16
F32 = jnp.float32
LANES = 128
TILE = 2 * LANES
PITCH = 129


def _encoder_kernel(dims, img, wd1, bd1, wc1, bc1, wd2, bd2, wc2, bc2, wd3, bd3, wc3, bc3, out,
                    raw, xt, y1, z1, y2, z2, y3, st0, st1, st2,
                    vwd1, vwc1, vwd2, vwc2, vwd3, vwc3, wp1, wp2, wp6,
                    vb1, vb2, vb3, vb4, vb5, vb6,
                    raw_sem, w_sem, rh_send, rh_recv, xc_send, xc_recv,
                    row_send, row_recv, cor_send, cor_recv, col_send, col_recv):
    row_len, col_len = dims
    nimg = img.shape[0]
    my_row = lax.axis_index('row')
    my_col = lax.axis_index('col')
    up, down = my_row > 0, my_row < row_len - 1
    left, right = my_col > 0, my_col < col_len - 1

    def both(a, b):
        return jnp.logical_and(a, b)

    near = [(up, -1, 0), (down, 1, 0), (left, 0, -1), (right, 0, 1)]
    near += [(both(v[0], g[0]), v[1], g[2]) for v in near[:2] for g in near[2:]]

    def dev(dr, dc):
        return {'row': my_row + dr, 'col': my_col + dc}

    def raw_copy(k):
        return pltpu.make_async_copy(img.at[:, pl.ds(2 * k - 1, 2)], raw.at[k], raw_sem.at[k])

    last = raw.shape[0] - 1
    mid = last // 2
    first_copy = pltpu.make_async_copy(img.at[:, pl.ds(0, 1)], raw.at[0, :, pl.ds(1, 1)], raw_sem.at[0])
    last_copy = pltpu.make_async_copy(img.at[:, pl.ds(2 * last - 1, 1)], raw.at[last, :, pl.ds(0, 1)], raw_sem.at[last])
    order = []
    for t in range(last - 1):
        h = (t + 1) // 2
        order.append(mid - h if t % 2 else mid + h)
    weights = [(wd1, vwd1), (wc1, vwc1), (wd2, vwd2), (wc2, vwc2), (wd3, vwd3), (wc3, vwc3),
               *((x, v.at[0]) for x, v in zip((bd1, bc1, bd2, bc2, bd3, bc3), (vb1, vb2, vb3, vb4, vb5, vb6)))]
    wcopies = [pltpu.make_async_copy(s, d, w_sem.at[i]) for i, (s, d) in enumerate(weights)]
    for i in (0, 6, 1, 7):
        wcopies[i].start()
    for k in order[:6]:
        raw_copy(k).start()

    barrier = pltpu.get_barrier_semaphore()
    for there, dr, dc in near:
        @pl.when(there)
        def _(dr=dr, dc=dc):
            pl.semaphore_signal(barrier, inc=1, device_id=dev(dr, dc), device_id_type=pl.DeviceIdType.MESH)
    nu, nd, nl, nr = [jnp.where(x, 1, 0) for x in (up, down, left, right)]
    pl.semaphore_wait(barrier, (1 + nu + nd) * (1 + nl + nr) - 1)

    def raw_send(s):
        if s == 0:
            return pltpu.make_async_remote_copy(img.at[:, pl.ds(0, 1)], raw.at[last, :, pl.ds(1, 1)],
                                                rh_send.at[0], rh_recv.at[0], device_id=dev(-1, 0), device_id_type=pl.DeviceIdType.MESH)
        return pltpu.make_async_remote_copy(img.at[:, pl.ds(2 * last - 1, 1)], raw.at[0, :, pl.ds(0, 1)],
                                            rh_send.at[1], rh_recv.at[1], device_id=dev(1, 0), device_id_type=pl.DeviceIdType.MESH)

    for there, s in zip((up, down), range(2)):
        @pl.when(there)
        def _(s=s):
            raw_send(s).start()

    def zero(ref):
        ref[...] = jnp.zeros(ref.shape, ref.dtype)

    def buf(ref, cut):
        h, u = ref.shape[0] - 2, ref.shape[1] - 2
        if len(ref.shape) > 4:
            where = dict(hl=(0, 1), first=(1, 0), last=(u, 1), hr=(u + 1, 0))
        else:
            where = dict(hl=(0,), first=(1,), last=(u,), hr=(u + 1,))
        return dict(ref=ref, h=h, spans=((0, cut), (cut, u - cut)), **where)

    bufs = []
    cut = (y1.shape[1] - 2) * 5 // 8
    for ref in (y1, z1, y2, z2, y3):
        bufs.append(buf(ref, cut))
        cut = (cut - 1) // 2 if ref is y2 else cut - 1

    for b in bufs:
        ref, h = b['ref'], b['h']

        @pl.when(jnp.logical_not(up))
        def _(ref=ref):
            zero(ref.at[0])

        @pl.when(jnp.logical_not(down))
        def _(ref=ref, h=h):
            zero(ref.at[h + 1])

        @pl.when(jnp.logical_not(left))
        def _(ref=ref, b=b, h=h):
            for r in range(h + 2):
                zero(ref.at[(r,) + b['hl']])

        @pl.when(jnp.logical_not(right))
        def _(ref=ref, b=b, h=h):
            for r in range(h + 2):
                zero(ref.at[(r,) + b['hr']])

    @pl.when(jnp.logical_not(up))
    def _():
        for n in range(nimg):
            zero(raw.at[0, n, 0])

    @pl.when(jnp.logical_not(down))
    def _():
        for n in range(nimg):
            zero(raw.at[last, n, 1])

    xu = xt.shape[1] - 2

    @pl.when(jnp.logical_not(left))
    def _():
        for k in range(last + 1):
            zero(xt.at[k, 0, 3])

    @pl.when(jnp.logical_not(right))
    def _():
        for k in range(last + 1):
            zero(xt.at[k, xu + 1, 0])

    def row_copy(i, s, part):
        b = bufs[i]
        c, w = b['spans'][part]
        ref, h = b['ref'], b['h']
        src, dst, dr = (1, h + 1, -1) if s == 0 else (h, 0, 1)
        return pltpu.make_async_remote_copy(ref.at[src, pl.ds(1 + c, w)], ref.at[dst, pl.ds(1 + c, w)], row_send.at[i, s, part], row_recv.at[i, s, part],
                                            device_id=dev(dr, 0), device_id_type=pl.DeviceIdType.MESH)

    def corner_copy(i, s):
        b = bufs[i]
        ref, h = b['ref'], b['h']
        dr, dc = near[4 + s][1:]
        src = (1 if dr < 0 else h,) + (b['first'] if dc < 0 else b['last'])
        dst = (h + 1 if dr < 0 else 0,) + (b['hr'] if dc < 0 else b['hl'])
        return pltpu.make_async_remote_copy(ref.at[src], ref.at[dst], cor_send.at[i, s], cor_recv.at[i, s],
                                            device_id=dev(dr, dc), device_id_type=pl.DeviceIdType.MESH)

    def col_copy(i, r, s):
        b = bufs[i]
        ref = b['ref']
        src, dst, dc = (b['first'], b['hr'], -1) if s == 0 else (b['last'], b['hl'], 1)
        return pltpu.make_async_remote_copy(ref.at[(r + 1,) + src], ref.at[(r + 1,) + dst], col_send.at[i, s], col_recv.at[i, r, s],
                                            device_id=dev(0, dc), device_id_type=pl.DeviceIdType.MESH)

    sides = ((left, 0), (right, 1))
    from_sides = ((right, 0), (left, 1))

    def each(cases, act):
        for there, s in cases:
            @pl.when(there)
            def _(s=s):
                act(s)

    ends = list(zip((up, down), range(2)))
    from_ends = list(zip((down, up), range(2)))
    corners = [(x[0], s) for s, x in enumerate(near[4:])]
    from_corners = [(x[0], s) for s, x in enumerate(near[:3:-1])]

    def send_rows(i, part):
        each(ends, lambda s: row_copy(i, s, part).start())
        each(corners[part::2], lambda s: corner_copy(i, s).start())

    def wait_rows(i, part):
        each(from_ends, lambda s: row_copy(i, s, part).wait_recv())
        each(from_corners[1 - part::2], lambda s: corner_copy(i, s).wait_recv())

    def xcol_copy(k, s):
        src, dst, dc = ((1, 0), (xu + 1, 0), -1) if s == 0 else ((xu, 3), (0, 3), 1)
        return pltpu.make_async_remote_copy(xt.at[(k,) + src], xt.at[(k,) + dst], xc_send.at[s], xc_recv.at[k, s],
                                            device_id=dev(0, dc), device_id_type=pl.DeviceIdType.MESH)

    def send_xcols(ks):
        each(sides, lambda s: [xcol_copy(k, s).start() for k in ks])

    def wait_xcols(*ks):
        each(from_sides, lambda s: [xcol_copy(k, s).wait_recv() for k in ks])

    for i in (0, 1, 6, 7):
        wcopies[i].wait()

    def loop(count, act):
        def body(i, carry):
            act(i)
            return carry
        lax.fori_loop(0, count, body, 0)

    def zero_block(ref):
        def act(i):
            zero(ref.at[i])
        return act

    def fill1(i):
        dk, dc, cpar, rpar = i // 8, i // 4 % 2, i // 2 % 2, i % 2
        for j in range(2):
            wp1[(dk * 3 + dc + j) * 4 + cpar * 2 + rpar, :, pl.ds(j * LANES, LANES)] = vwd1[2 * dk + rpar, 2 * dc + cpar]

    def fill2(i):
        for j in range(2):
            wp2[i // 3 * 4 + i % 3 + j, :, pl.ds(j * LANES, LANES)] = vwc1[i // 3, i % 3]

    loop(wp1.shape[0], zero_block(wp1))
    loop(wp2.shape[0], zero_block(wp2))
    loop(16, fill1)
    loop(9, fill2)

    eye = (lax.broadcasted_iota(jnp.int32, (LANES, LANES), 0) == lax.broadcasted_iota(jnp.int32, (LANES, LANES), 1)).astype(F32).astype(BF)

    def transpose_in(k, st):
        for s in range(nimg // 2):
            rhs = raw[k, pl.ds(2 * s, 2)].reshape(TILE, LANES)
            t = lax.dot_general(eye, rhs, BY_LAST, preferred_element_type=F32)
            st[pl.ds(2 * s * PITCH, LANES), :] = t[:, :LANES]
            st[pl.ds((2 * s + 1) * PITCH, LANES), :] = t[:, LANES:]

    def transpose_out(k, st):
        for c in range(4 * xu):
            xt[k, 1 + c // 4, c % 4] = st[pl.ds(c, nimg, stride=PITCH), :].astype(BF)

    def middle_out(t):
        h = (t + 1) // 2
        return mid + h * (1 - 2 * (t % 2))

    inner = (last - 1) // 3

    def take_three(it, carry):
        edge = it // inner
        ks = [edge * (last * min(d, 1)) + (1 - edge) * middle_out(3 * it + d) for d in range(3)]

        @pl.when(it < inner - 2)
        def _():
            for d in range(3):
                raw_copy(middle_out(3 * it + 6 + d)).start()

        @pl.when(it == inner - 2)
        def _():
            first_copy.start()
            last_copy.start()

        @pl.when(it < inner)
        def _():
            for k in ks:
                raw_copy(k).wait()

        @pl.when(it == inner)
        def _():
            first_copy.wait()
            last_copy.wait()
            each(from_ends, lambda s: raw_send(s).wait_recv())
        for k, st in zip(ks, (st0, st1, st2)):
            transpose_in(k, st)
        for k, st in zip(ks, (st0, st1, st2)):
            transpose_out(k, st)
        send_xcols(ks[:2])

        @pl.when(it < inner)
        def _():
            send_xcols(ks[2:])
        return carry

    def finish(acc, bias):
        return jnp.maximum(acc + bias, 0.0).astype(BF)

    def put_pairs(ref, i, c, w, v):
        for j in range(2):
            ref[i + 1, pl.ds(1 + c, w), j] = v[:, j * LANES:(j + 1) * LANES].reshape(w, nimg, LANES)

    def strips_dot(group, taps, dot, put):
        lhs = [jnp.concatenate([tap(*strip) for strip in group], axis=0) for tap in taps]
        v = dot(jnp.concatenate(lhs, axis=-1))
        at = 0
        for i, c, w in group:
            m = v.shape[0] * w // sum(strip[2] for strip in group)
            put(i, c, w, v[at:at + m])
            at += m

    def rows_of(ref, idx, w):
        v = ref[idx]
        return v.reshape(w * nimg, v.shape[-1])

    def wait_pair(i, a, h):
        each(from_sides, lambda s: [col_copy(i, r, s).wait_recv() for r in (a, h - 1 - a)])

    def step_of(t, n, p):
        up_now = (t + n - p) // n
        return (1 - up_now) * (n - 1 - t) + up_now * (t - p)

    def conv_waits(i, p):
        h = bufs[i]['h']
        n = h // 2
        seen = n - 1 - p if p else n

        def waits(t, a):
            if p:
                @pl.when(t == 0)
                def _():
                    wait_pair(i, n - 1, h)

                @pl.when(t < p)
                def _():
                    wait_pair(i, a - 1, h)

            @pl.when((t > p) & (a + 1 < seen))
            def _():
                wait_pair(i, a + 1, h)

        def edge_waits():
            wait_pair(i, 0, h)
            wait_pair(i, 1, h)
        return waits, edge_waits, lambda part: wait_rows(i, part)

    def down_waits(i):
        h = bufs[i]['h']

        def waits(t, a):
            wait_pair(i, 2 * a + 1, h)

            @pl.when(a < h // 4 - 1)
            def _():
                wait_pair(i, 2 * a + 2, h)

        def edge_waits():
            for r in range(3):
                wait_pair(i, r, h)
        return waits, edge_waits, lambda part: wait_rows(i, part)

    def run(made):
        body, count = made
        lax.fori_loop(0, count, body, 0)

    pairs = y1.shape[1] - 2
    bias1 = jnp.concatenate([vb1[...], vb1[...]], axis=-1)
    h1 = y1.shape[0] - 2

    e1 = 4

    def down1_waits(t, a):
        @pl.when(t == 0)
        def _():
            wait_xcols(mid)

        @pl.when(t < e1)
        def _():
            wait_xcols(a, last - a)

        @pl.when((t > e1) & (a + 1 < h1 // 2 - e1))
        def _():
            wait_xcols(a + 1, last - 1 - a)

    def layer(i, p, waits, edge_waits, part_waits, taps, dot, put, join=False):
        b = bufs[i]
        h = b['h']
        width = sum(b['spans'][1])

        def body(t, carry):
            a = step_of(t, h // 2, p)

            @pl.when(t != p)
            def _():
                waits(t, a)
                group = [(a, 0, width), (h - 1 - a, 0, width)]
                for g in [group] if join else [group[:1], group[1:]]:
                    strips_dot(g, taps, dot, put)
                each(sides, lambda s: [col_copy(i, r, s).start() for r in (a, h - 1 - a)])

            @pl.when(t == p)
            def _():
                edge_waits()
                for part in range(2):
                    part_waits(part)
                    strips_dot([(r, *b['spans'][part]) for r in (0, h - 1)], taps, dot, put)
                    send_rows(i, part)
                    each(sides[part:part + 1], lambda s: [col_copy(i, r, s).start() for r in (0, h - 1)])
            return carry
        return body, h // 2

    def tap_of(ref, stride, p, s):
        if len(ref.shape) > 4:
            return lambda i, c, w: rows_of(ref, (stride * i + p, pl.ds(c + (s + 1) // 2, w), (s + 1) % 2), w)
        return lambda i, c, w: rows_of(ref, (i + p, pl.ds(c + s, w)), w)

    def relu_dot(weight, bias):
        return lambda lhs: finish(jnp.dot(lhs, weight(), preferred_element_type=F32), bias)

    def image_tap(dk, p):
        return lambda i, c, w: rows_of(xt, (i + dk, pl.ds(c + p // 4, w), p % 4), w)

    down1, _ = layer(0, e1, down1_waits, lambda: wait_xcols(0, last, 1, last - 1), lambda part: None,
                     [image_tap(dk, p) for dk in range(2) for p in range(3, 9)],
                     relu_dot(lambda: wp1[...].reshape(6 * TILE, TILE), bias1), functools.partial(put_pairs, y1))

    def phase(ph, carry):
        lax.fori_loop(inner * ph, inner + ph, take_three, 0)

        @pl.when(ph == 0)
        def _():
            for i in range(2, 6):
                wcopies[i].start()
                wcopies[i + 6].start()
        lax.fori_loop((e1 - 2) * ph, e1 - 2 + (h1 // 2 - e1 + 2) * ph, down1, 0)
        return carry

    lax.fori_loop(0, 2, phase, 0)

    bias2 = jnp.concatenate([vb2[...], vb2[...]], axis=-1)

    run(layer(1, 2, *conv_waits(0, 2), [tap_of(y1, 1, p, s) for p in range(3) for s in range(4)],
              relu_dot(lambda: wp2[...].reshape(6 * TILE, TILE), bias2), functools.partial(put_pairs, z1)))

    ch3 = out.shape[-1]
    h2 = y2.shape[0] - 2
    w2 = y2.shape[1] - 2
    for i in (2, 8):
        wcopies[i].wait()

    def put_flat(ref, i, c, w, v):
        ref[i + 1, pl.ds(1 + c, w)] = v.reshape(w, nimg, v.shape[-1])

    run(layer(2, 0, *down_waits(1), [tap_of(z1, 2, p, s) for p in range(4) for s in range(4)],
              relu_dot(lambda: vwd2[...].reshape(16 * LANES, TILE), vb3[...]), functools.partial(put_flat, y2)))
    for i in (3, 9, 5):
        wcopies[i].wait()

    def fill6(i):
        wp6[i, pl.ds(0, ch3), :] = vwc3[i // 3, i % 3]
        wp6[i, pl.ds(ch3, wp6.shape[1] - ch3), :] = jnp.zeros((wp6.shape[1] - ch3, ch3), BF)

    loop(9, fill6)

    def put_even_odd(i, c, w, v):
        v = v.reshape(w, 2, nimg, v.shape[-1])
        for j in range(2):
            z2[i + 1, pl.ds(1 + c, w), j] = v[:, j]

    def pair_tap(p, q):
        return lambda i, c, w: rows_of(y2, (i + p, pl.ds(2 * c + q, 2 * w)), 2 * w)

    run(layer(3, 0, *conv_waits(2, 0), [pair_tap(p, q) for p in range(3) for q in range(3)],
              relu_dot(lambda: vwc2[...].reshape(9 * TILE, TILE), vb4[...]), put_even_odd))

    h3 = y3.shape[0] - 2
    w3 = y3.shape[1] - 2
    for i in (4, 10, 11):
        wcopies[i].wait()

    def down3_dot(lhs):
        wts = jnp.concatenate([vwd3[p, q] for p in range(4) for q in range(4)], axis=-1)
        v = finish(lax.dot_general(lhs, wts, BY_LAST, preferred_element_type=F32), vb5[...])
        return jnp.concatenate([v, jnp.zeros((v.shape[0], y3.shape[-1] - ch3), BF)], axis=-1)

    run(layer(4, 0, *down_waits(3), [tap_of(z2, 2, p, s) for p in range(4) for s in range(4)],
              down3_dot, functools.partial(put_flat, y3), join=True))

    def conv3(t, carry):
        @pl.when(t == 1)
        def _():
            for r in range(h3 // 2):
                wait_pair(4, r, h3)
            for part in range(2):
                wait_rows(4, part)
        top, bottom, lo, hi = 1 - t, h3 - 2 + t, 1 - t, w3 - 2 + t
        strips = [(i, 1, w3 - 2) for i in (top, bottom)] + [(i, c, 1) for i in (top, bottom, *range(1, h3 - 1)) for c in (lo, hi)]
        parts = []
        for p in range(3):
            for q in range(3):
                parts.append(jnp.concatenate([rows_of(y3, (i + p, pl.ds(c + q, w)), w) for i, c, w in strips], axis=0))
        acc = jnp.dot(jnp.concatenate(parts, axis=-1), wp6[...].reshape(9 * wp6.shape[1], ch3), preferred_element_type=F32)
        v = finish(acc, vb6[...])
        at = 0
        for i, c, w in strips:
            out[i, pl.ds(c, w)] = v[at:at + w * nimg].reshape(w, nimg, ch3)
            at += w * nimg
        return carry

    lax.fori_loop(0, 2, conv3, 0)

    each(ends, lambda s: raw_send(s).wait_send())

    def drain_cols(ref, rows, at, sem):
        whole = ref.at[(rows,) + at]
        pltpu.make_async_remote_copy(whole, whole, sem, sem, device_id=dev(0, 0), device_id_type=pl.DeviceIdType.MESH).wait_send()

    each(sides, lambda s: drain_cols(xt, pl.ds(0, last + 1), (1, 0), xc_send.at[s]))
    for i, b in enumerate(bufs):
        for part in range(2):
            each(ends, lambda s: row_copy(i, s, part).wait_send())
        each(corners, lambda s: corner_copy(i, s).wait_send())
        each(sides, lambda s: drain_cols(b['ref'], pl.ds(1, b['h']), b['first'], col_send.at[i, s]))


def solution(mesh):
    dims = (mesh.shape['row'], mesh.shape['col'])

    def local_encoder(images, w_down1, b_down1, w_conv1, b_conv1, w_down2, b_down2, w_conv2, b_conv2, w_down3, b_down3, w_conv3, b_conv3):
        n, h, w, c = images.shape
        img = jnp.transpose(images, (0, 1, 3, 2))
        wd3 = jnp.transpose(w_down3, (0, 1, 3, 2))
        c1, c2, c3 = w_conv1.shape[-1], w_conv2.shape[-1], w_conv3.shape[-1]
        c3p = pl.cdiv(c3, LANES) * LANES
        hbm = pl.BlockSpec(memory_space=pl.ANY)
        dma = pltpu.SemaphoreType.DMA
        hh, hq, he = h // 2, h // 4, h // 8
        wq, we = w // 4, w // 8
        kk = hh + 1
        scratch = [
            pltpu.VMEM((kk, n, 2, c, w), BF),
            pltpu.VMEM((kk, wq + 2, 4, n, 2 * c), BF),
            pltpu.VMEM((hh + 2, wq + 2, 2, n, c1), BF),
            pltpu.VMEM((hh + 2, wq + 2, 2, n, c1), BF),
            pltpu.VMEM((hq + 2, wq + 2, n, c2), BF),
            pltpu.VMEM((hq + 2, we + 2, 2, n, c2), BF),
            pltpu.VMEM((he + 2, we + 2, n, c3p), BF),
        ] + [pltpu.VMEM((n * PITCH, LANES), F32)] * 3 + [
            pltpu.VMEM(x.shape, BF) for x in (w_down1, w_conv1, w_down2, w_conv2, wd3, w_conv3)
        ] + [
            pltpu.VMEM((24, c, TILE), BF),
            pltpu.VMEM((12, c1, TILE), BF),
            pltpu.VMEM((9, c3p, c3), BF),
        ] + [pltpu.VMEM((1, k), F32) for k in (c1, c1, c2, c2, c3, c3)] + [
            dma(d) for d in ((kk,), (12,), (2,), (2,), (2,), (kk, 2), (5, 2, 2), (5, 2, 2), (5, 4), (5, 4), (5, 2), (5, hh, 2))
        ]
        feats = pl.pallas_call(
            functools.partial(_encoder_kernel, dims),
            out_shape=jax.ShapeDtypeStruct((he, we, n, c3), BF),
            in_specs=[hbm] * 13,
            out_specs=pl.BlockSpec(memory_space=pltpu.VMEM),
            scratch_shapes=scratch,
            compiler_params=pltpu.CompilerParams(collective_id=0, has_side_effects=True, vmem_limit_bytes=62 * 1024 * 1024),
        )(img, w_down1, b_down1, w_conv1, b_conv1, w_down2, b_down2, w_conv2, b_conv2, wd3, b_down3, w_conv3, b_conv3)
        return jnp.transpose(feats, (2, 0, 1, 3))

    tile_spec = P('batch', 'row', 'col', None)
    return jax.shard_map(local_encoder, mesh=mesh, in_specs=(tile_spec,) + (P(),) * 12, out_specs=tile_spec, check_vma=False)
```

```python
import functools

import jax
import jax.numpy as jnp
from jax import lax
from jax.experimental import pallas as pl
from jax.experimental.pallas import tpu as pltpu
from jax.sharding import PartitionSpec as P

BY_LAST = (((1,), (1,)), ((), ()))
BF = jnp.bfloat16
F32 = jnp.float32
LANES = 128
TILE = 2 * LANES
PITCH = 129


def _encoder_kernel(dims, img, wd1, bd1, wc1, bc1, wd2, bd2, wc2, bc2, wd3, bd3, wc3, bc3, out,
                    raw, xt, y1, z1, y2, z2, y3, st0, st1, st2,
                    vwd1, vwc1, vwd2, vwc2, vwd3, vwc3, wp1, wp2, wp6,
                    vb1, vb2, vb3, vb4, vb5, vb6,
                    raw_sem, w_sem, rh_send, rh_recv, xc_send, xc_recv,
                    row_send, row_recv, cor_send, cor_recv, col_send, col_recv):
    row_len, col_len = dims
    nimg = img.shape[0]
    my_row = lax.axis_index('row')
    my_col = lax.axis_index('col')
    up, down = my_row > 0, my_row < row_len - 1
    left, right = my_col > 0, my_col < col_len - 1

    def both(a, b):
        return jnp.logical_and(a, b)

    near = [(up, -1, 0), (down, 1, 0), (left, 0, -1), (right, 0, 1)]
    near += [(both(v[0], g[0]), v[1], g[2]) for v in near[:2] for g in near[2:]]

    def dev(dr, dc):
        return {'row': my_row + dr, 'col': my_col + dc}

    def raw_copy(k):
        return pltpu.make_async_copy(img.at[:, pl.ds(2 * k - 1, 2)], raw.at[k], raw_sem.at[k])

    last = raw.shape[0] - 1
    mid = last // 2
    first_copy = pltpu.make_async_copy(img.at[:, pl.ds(0, 1)], raw.at[0, :, pl.ds(1, 1)], raw_sem.at[0])
    last_copy = pltpu.make_async_copy(img.at[:, pl.ds(2 * last - 1, 1)], raw.at[last, :, pl.ds(0, 1)], raw_sem.at[last])
    def loop(count, act):
        def body(i, carry):
            act(i)
            return carry
        lax.fori_loop(0, count, body, 0)

    def middle_out(t):
        h = (t + 1) // 2
        return mid + h * (1 - 2 * (t % 2))

    weights = [(wd1, vwd1), (wc1, vwc1), (wd2, vwd2), (wc2, vwc2), (wd3, vwd3), (wc3, vwc3),
               *((x, v.at[0]) for x, v in zip((bd1, bc1, bd2, bc2, bd3, bc3), (vb1, vb2, vb3, vb4, vb5, vb6)))]
    wcopies = [pltpu.make_async_copy(s, d, w_sem.at[i]) for i, (s, d) in enumerate(weights)]
    for i in (0, 6, 1, 7):
        wcopies[i].start()
    loop(last - 1, lambda t: raw_copy(middle_out(t)).start())
    first_copy.start()
    last_copy.start()

    barrier = pltpu.get_barrier_semaphore()
    for there, dr, dc in near:
        @pl.when(there)
        def _(dr=dr, dc=dc):
            pl.semaphore_signal(barrier, inc=1, device_id=dev(dr, dc), device_id_type=pl.DeviceIdType.MESH)
    nu, nd, nl, nr = [jnp.where(x, 1, 0) for x in (up, down, left, right)]
    pl.semaphore_wait(barrier, (1 + nu + nd) * (1 + nl + nr) - 1)

    def raw_send(s):
        if s == 0:
            return pltpu.make_async_remote_copy(img.at[:, pl.ds(0, 1)], raw.at[last, :, pl.ds(1, 1)],
                                                rh_send.at[0], rh_recv.at[0], device_id=dev(-1, 0), device_id_type=pl.DeviceIdType.MESH)
        return pltpu.make_async_remote_copy(img.at[:, pl.ds(2 * last - 1, 1)], raw.at[0, :, pl.ds(0, 1)],
                                            rh_send.at[1], rh_recv.at[1], device_id=dev(1, 0), device_id_type=pl.DeviceIdType.MESH)

    for there, s in zip((up, down), range(2)):
        @pl.when(there)
        def _(s=s):
            raw_send(s).start()

    def zero(ref):
        ref[...] = jnp.zeros(ref.shape, ref.dtype)

    def wide(ref, h):
        u = ref.shape[1] - 2
        return dict(ref=ref, h=h, hl=(0, 1), first=(1, 0), last=(u, 1), hr=(u + 1, 0), real=pl.ds(1, u))

    def flat(ref, h):
        w = ref.shape[1] - 2
        return dict(ref=ref, h=h, hl=(0,), first=(1,), last=(w,), hr=(w + 1,), real=pl.ds(1, w))

    bufs = [wide(y1, y1.shape[0] - 2), wide(z1, z1.shape[0] - 2), flat(y2, y2.shape[0] - 2), wide(z2, z2.shape[0] - 2),
            flat(y3, y3.shape[0] - 2)]

    for b in bufs:
        ref, h = b['ref'], b['h']

        @pl.when(jnp.logical_not(up))
        def _(ref=ref):
            zero(ref.at[0])

        @pl.when(jnp.logical_not(down))
        def _(ref=ref, h=h):
            zero(ref.at[h + 1])

        @pl.when(jnp.logical_not(left))
        def _(ref=ref, b=b, h=h):
            for r in range(h + 2):
                zero(ref.at[(r,) + b['hl']])

        @pl.when(jnp.logical_not(right))
        def _(ref=ref, b=b, h=h):
            for r in range(h + 2):
                zero(ref.at[(r,) + b['hr']])

    @pl.when(jnp.logical_not(up))
    def _():
        for n in range(nimg):
            zero(raw.at[0, n, 0])

    @pl.when(jnp.logical_not(down))
    def _():
        for n in range(nimg):
            zero(raw.at[last, n, 1])

    xu = xt.shape[1] - 2

    @pl.when(jnp.logical_not(left))
    def _():
        for k in range(last + 1):
            zero(xt.at[k, 0, 3])

    @pl.when(jnp.logical_not(right))
    def _():
        for k in range(last + 1):
            zero(xt.at[k, xu + 1, 0])

    def row_copy(i, s):
        b = bufs[i]
        ref, h = b['ref'], b['h']
        src, dst, dr = (1, h + 1, -1) if s == 0 else (h, 0, 1)
        return pltpu.make_async_remote_copy(ref.at[src, b['real']], ref.at[dst, b['real']], row_send.at[i, s], row_recv.at[i, s],
                                            device_id=dev(dr, 0), device_id_type=pl.DeviceIdType.MESH)

    def corner_copy(i, s):
        b = bufs[i]
        ref, h = b['ref'], b['h']
        dr, dc = near[4 + s][1:]
        src = (1 if dr < 0 else h,) + (b['first'] if dc < 0 else b['last'])
        dst = (h + 1 if dr < 0 else 0,) + (b['hr'] if dc < 0 else b['hl'])
        return pltpu.make_async_remote_copy(ref.at[src], ref.at[dst], cor_send.at[i, s], cor_recv.at[i, s],
                                            device_id=dev(dr, dc), device_id_type=pl.DeviceIdType.MESH)

    def col_copy(i, r, s):
        b = bufs[i]
        ref = b['ref']
        src, dst, dc = (b['first'], b['hr'], -1) if s == 0 else (b['last'], b['hl'], 1)
        return pltpu.make_async_remote_copy(ref.at[(r + 1,) + src], ref.at[(r + 1,) + dst], col_send.at[i, s], col_recv.at[i, r, s],
                                            device_id=dev(0, dc), device_id_type=pl.DeviceIdType.MESH)

    sides = ((left, 0), (right, 1))
    from_sides = ((right, 0), (left, 1))

    def each(cases, act):
        for there, s in cases:
            @pl.when(there)
            def _(s=s):
                act(s)

    ends = list(zip((up, down), range(2)))
    from_ends = list(zip((down, up), range(2)))
    corners = [(x[0], s) for s, x in enumerate(near[4:])]
    from_corners = [(x[0], s) for s, x in enumerate(near[:3:-1])]

    def send_rows(i):
        each(ends, lambda s: row_copy(i, s).start())
        each(corners, lambda s: corner_copy(i, s).start())

    def wait_rows(i):
        each(from_ends, lambda s: row_copy(i, s).wait_recv())
        each(from_corners, lambda s: corner_copy(i, s).wait_recv())

    def xcol_copy(k, s):
        src, dst, dc = ((1, 0), (xu + 1, 0), -1) if s == 0 else ((xu, 3), (0, 3), 1)
        return pltpu.make_async_remote_copy(xt.at[(k,) + src], xt.at[(k,) + dst], xc_send.at[s], xc_recv.at[k, s],
                                            device_id=dev(0, dc), device_id_type=pl.DeviceIdType.MESH)

    def send_xcols(ks):
        each(sides, lambda s: [xcol_copy(k, s).start() for k in ks])

    def wait_xcols(*ks):
        each(from_sides, lambda s: [xcol_copy(k, s).wait_recv() for k in ks])

    for i in (0, 1, 6, 7):
        wcopies[i].wait()

    def zero_block(ref):
        def act(i):
            zero(ref.at[i])
        return act

    def fill1(i):
        dk, dc, cpar, rpar = i // 8, i // 4 % 2, i // 2 % 2, i % 2
        for j in range(2):
            wp1[(dk * 3 + dc + j) * 4 + cpar * 2 + rpar, :, pl.ds(j * LANES, LANES)] = vwd1[2 * dk + rpar, 2 * dc + cpar]

    def fill2(i):
        for j in range(2):
            wp2[i // 3 * 4 + i % 3 + j, :, pl.ds(j * LANES, LANES)] = vwc1[i // 3, i % 3]

    loop(wp1.shape[0], zero_block(wp1))
    loop(wp2.shape[0], zero_block(wp2))
    loop(16, fill1)
    loop(9, fill2)

    eye = (lax.broadcasted_iota(jnp.int32, (LANES, LANES), 0) == lax.broadcasted_iota(jnp.int32, (LANES, LANES), 1)).astype(F32).astype(BF)

    def transpose_in(k, st):
        for s in range(nimg // 2):
            rhs = raw[k, pl.ds(2 * s, 2)].reshape(TILE, LANES)
            t = lax.dot_general(eye, rhs, BY_LAST, preferred_element_type=F32)
            st[pl.ds(2 * s * PITCH, LANES), :] = t[:, :LANES]
            st[pl.ds((2 * s + 1) * PITCH, LANES), :] = t[:, LANES:]

    def transpose_out(k, st):
        for c in range(4 * xu):
            xt[k, 1 + c // 4, c % 4] = st[pl.ds(c, nimg, stride=PITCH), :].astype(BF)

    inner = (last - 1) // 3

    def take_three(it, carry):
        edge = it // inner
        ks = [edge * (last * min(d, 1)) + (1 - edge) * middle_out(3 * it + d) for d in range(3)]

        @pl.when(it < inner)
        def _():
            for k in ks:
                raw_copy(k).wait()

        @pl.when(it == inner)
        def _():
            first_copy.wait()
            last_copy.wait()
            each(from_ends, lambda s: raw_send(s).wait_recv())
        for k, st in zip(ks, (st0, st1, st2)):
            transpose_in(k, st)
        for k, st in zip(ks, (st0, st1, st2)):
            transpose_out(k, st)
        send_xcols(ks[:2])

        @pl.when(it < inner)
        def _():
            send_xcols(ks[2:])
        return carry

    def finish(acc, bias):
        return jnp.maximum(acc + bias, 0.0).astype(BF)

    def put_pairs(ref, i, v):
        for j in range(2):
            ref[i + 1, pl.ds(1, pairs), j] = v[:, j * LANES:(j + 1) * LANES].reshape(pairs, nimg, LANES)

    def rows_of(ref, idx, w):
        v = ref[idx]
        return v.reshape(w * nimg, v.shape[-1])

    def wait_pair(i, a, h):
        each(from_sides, lambda s: [col_copy(i, r, s).wait_recv() for r in (a, h - 1 - a)])

    def step_of(t, n, p):
        up_now = (t + n - p) // n
        return (1 - up_now) * (n - 1 - t) + up_now * (t - p)

    def wait_conv(i, t, a, h, p):
        n = h // 2
        seen = n - 1 - p if p else n

        if p:
            @pl.when(t == 0)
            def _():
                wait_pair(i, n - 1, h)

            @pl.when(t < p)
            def _():
                wait_pair(i, a - 1, h)

        @pl.when(t == p)
        def _():
            wait_pair(i, 0, h)
            wait_rows(i)

        @pl.when(jnp.logical_and(t >= p, a + 1 < seen))
        def _():
            wait_pair(i, a + 1, h)

    def wait_down(i, a, h):
        @pl.when(a == 0)
        def _():
            wait_pair(i, 0, 2 * h)
            wait_rows(i)
        wait_pair(i, 2 * a + 1, 2 * h)

        @pl.when(a < h // 2 - 1)
        def _():
            wait_pair(i, 2 * a + 2, 2 * h)

    def send(i, t, a, h, e):
        @pl.when(t == e)
        def _():
            send_rows(i)
        each(sides, lambda s: [col_copy(i, r, s).start() for r in (a, h - 1 - a)])

    pairs = y1.shape[1] - 2
    bias1 = jnp.concatenate([vb1[...], vb1[...]], axis=-1)
    h1 = y1.shape[0] - 2

    e1 = 4

    def down1(t, carry):
        a = step_of(t, h1 // 2, e1)

        @pl.when(t == 0)
        def _():
            wait_xcols(mid)

        @pl.when(t < e1)
        def _():
            wait_xcols(a, last - a)

        @pl.when(t == e1)
        def _():
            wait_xcols(0, last)

        @pl.when(jnp.logical_and(t >= e1, a + 1 < h1 // 2 - e1))
        def _():
            wait_xcols(a + 1, last - 1 - a)
        for i in (a, h1 - 1 - a):
            parts = []
            for dk in range(2):
                for p in range(3, 9):
                    parts.append(rows_of(xt, (i + dk, pl.ds(p // 4, pairs), p % 4), pairs))
            acc = jnp.dot(jnp.concatenate(parts, axis=-1), wp1[...].reshape(6 * TILE, TILE), preferred_element_type=F32)
            v = finish(acc, bias1)
            put_pairs(y1, i, v)
        send(0, t, a, h1, e1)
        return carry

    def phase(ph, carry):
        lax.fori_loop(inner * ph, inner + ph, take_three, 0)

        @pl.when(ph == 0)
        def _():
            for i in range(2, 6):
                wcopies[i].start()
                wcopies[i + 6].start()
        lax.fori_loop((e1 - 2) * ph, e1 - 2 + (h1 // 2 - e1 + 2) * ph, down1, 0)
        return carry

    lax.fori_loop(0, 2, phase, 0)

    bias2 = jnp.concatenate([vb2[...], vb2[...]], axis=-1)

    def conv1(t, carry):
        a = step_of(t, h1 // 2, 2)
        wait_conv(0, t, a, h1, 2)
        for i in (a, h1 - 1 - a):
            parts = []
            for p in range(3):
                for s in range(1, 5):
                    parts.append(rows_of(y1, (i + p, pl.ds(s // 2, pairs), s % 2), pairs))
            acc = jnp.dot(jnp.concatenate(parts, axis=-1), wp2[...].reshape(6 * TILE, TILE), preferred_element_type=F32)
            v = finish(acc, bias2)
            put_pairs(z1, i, v)
        send(1, t, a, h1, 2)
        return carry

    lax.fori_loop(0, h1 // 2, conv1, 0)

    ch3 = out.shape[-1]
    h2 = y2.shape[0] - 2
    w2 = y2.shape[1] - 2
    for i in (2, 8):
        wcopies[i].wait()

    def down2(t, carry):
        a = t
        wait_down(1, a, h2)
        for i in (a, h2 - 1 - a):
            parts = []
            for p in range(4):
                for s in range(1, 5):
                    parts.append(rows_of(z1, (2 * i + p, pl.ds(s // 2, w2), s % 2), w2))
            acc = jnp.dot(jnp.concatenate(parts, axis=-1), vwd2[...].reshape(16 * LANES, TILE), preferred_element_type=F32)
            y2[i + 1, pl.ds(1, w2)] = finish(acc, vb3[...]).reshape(w2, nimg, TILE)
        send(2, t, a, h2, 0)
        return carry

    lax.fori_loop(0, h2 // 2, down2, 0)
    for i in (3, 9, 5):
        wcopies[i].wait()

    def fill6(i):
        wp6[i, pl.ds(0, ch3), :] = vwc3[i // 3, i % 3]
        wp6[i, pl.ds(ch3, wp6.shape[1] - ch3), :] = jnp.zeros((wp6.shape[1] - ch3, ch3), BF)

    loop(9, fill6)

    def conv2(t, carry):
        a = t
        wait_conv(2, t, a, h2, 0)
        for i in (a, h2 - 1 - a):
            parts = []
            for p in range(3):
                for q in range(3):
                    parts.append(rows_of(y2, (i + p, pl.ds(q, w2)), w2))
            acc = jnp.dot(jnp.concatenate(parts, axis=-1), vwc2[...].reshape(9 * TILE, TILE), preferred_element_type=F32)
            v = finish(acc, vb4[...]).reshape(w2 // 2, 2, nimg, TILE)
            z2[i + 1, pl.ds(1, w2 // 2), 0] = v[:, 0]
            z2[i + 1, pl.ds(1, w2 // 2), 1] = v[:, 1]
        send(3, t, a, h2, 0)
        return carry

    lax.fori_loop(0, h2 // 2, conv2, 0)

    h3 = y3.shape[0] - 2
    w3 = y3.shape[1] - 2
    for i in (4, 10, 11):
        wcopies[i].wait()

    def down3(t, carry):
        a = t
        wait_down(3, a, h3)
        ii = (a, h3 - 1 - a)
        parts, wts = [], []
        for p in range(4):
            for s in range(1, 5):
                parts.append(jnp.concatenate([rows_of(z2, (2 * i + p, pl.ds(s // 2, w3), s % 2), w3) for i in ii], axis=0))
                wts.append(vwd3[p, s - 1])
        acc = lax.dot_general(jnp.concatenate(parts, axis=-1), jnp.concatenate(wts, axis=-1), BY_LAST, preferred_element_type=F32)
        v = finish(acc, vb5[...])
        v = jnp.concatenate([v, jnp.zeros((v.shape[0], y3.shape[-1] - ch3), BF)], axis=-1)
        for n, i in enumerate(ii):
            y3[i + 1, pl.ds(1, w3)] = v[n * w3 * nimg:(n + 1) * w3 * nimg].reshape(w3, nimg, y3.shape[-1])
        send(4, t, a, h3, 0)
        return carry

    lax.fori_loop(0, h3 // 2, down3, 0)

    def conv3(t, carry):
        @pl.when(t == 1)
        def _():
            for r in range(h3 // 2):
                wait_pair(4, r, h3)
            wait_rows(4)
        top, bottom, lo, hi = 1 - t, h3 - 2 + t, 1 - t, w3 - 2 + t
        strips = [(i, 1, w3 - 2) for i in (top, bottom)] + [(i, c, 1) for i in (top, bottom, *range(1, h3 - 1)) for c in (lo, hi)]
        parts = []
        for p in range(3):
            for q in range(3):
                parts.append(jnp.concatenate([rows_of(y3, (i + p, pl.ds(c + q, w)), w) for i, c, w in strips], axis=0))
        acc = jnp.dot(jnp.concatenate(parts, axis=-1), wp6[...].reshape(9 * wp6.shape[1], ch3), preferred_element_type=F32)
        v = finish(acc, vb6[...])
        at = 0
        for i, c, w in strips:
            out[i, pl.ds(c, w)] = v[at:at + w * nimg].reshape(w, nimg, ch3)
            at += w * nimg
        return carry

    lax.fori_loop(0, 2, conv3, 0)

    each(ends, lambda s: raw_send(s).wait_send())

    def drain_cols(ref, rows, at, sem):
        whole = ref.at[(rows,) + at]
        pltpu.make_async_remote_copy(whole, whole, sem, sem, device_id=dev(0, 0), device_id_type=pl.DeviceIdType.MESH).wait_send()

    each(sides, lambda s: drain_cols(xt, pl.ds(0, last + 1), (1, 0), xc_send.at[s]))
    for i, b in enumerate(bufs):
        each(ends, lambda s: row_copy(i, s).wait_send())
        each(corners, lambda s: corner_copy(i, s).wait_send())
        each(sides, lambda s: drain_cols(b['ref'], pl.ds(1, b['h']), b['first'], col_send.at[i, s]))


def solution(mesh):
    dims = (mesh.shape['row'], mesh.shape['col'])

    def local_encoder(images, w_down1, b_down1, w_conv1, b_conv1, w_down2, b_down2, w_conv2, b_conv2, w_down3, b_down3, w_conv3, b_conv3):
        n, h, w, c = images.shape
        img = jnp.transpose(images, (0, 1, 3, 2))
        wd3 = jnp.transpose(w_down3, (0, 1, 3, 2))
        c1, c2, c3 = w_conv1.shape[-1], w_conv2.shape[-1], w_conv3.shape[-1]
        c3p = pl.cdiv(c3, LANES) * LANES
        hbm = pl.BlockSpec(memory_space=pl.ANY)
        dma = pltpu.SemaphoreType.DMA
        hh, hq, he = h // 2, h // 4, h // 8
        wq, we = w // 4, w // 8
        kk = hh + 1
        scratch = [
            pltpu.VMEM((kk, n, 2, c, w), BF),
            pltpu.VMEM((kk, wq + 2, 4, n, 2 * c), BF),
            pltpu.VMEM((hh + 2, wq + 2, 2, n, c1), BF),
            pltpu.VMEM((hh + 2, wq + 2, 2, n, c1), BF),
            pltpu.VMEM((hq + 2, wq + 2, n, c2), BF),
            pltpu.VMEM((hq + 2, we + 2, 2, n, c2), BF),
            pltpu.VMEM((he + 2, we + 2, n, c3p), BF),
        ] + [pltpu.VMEM((n * PITCH, LANES), F32)] * 3 + [
            pltpu.VMEM(x.shape, BF) for x in (w_down1, w_conv1, w_down2, w_conv2, wd3, w_conv3)
        ] + [
            pltpu.VMEM((24, c, TILE), BF),
            pltpu.VMEM((12, c1, TILE), BF),
            pltpu.VMEM((9, c3p, c3), BF),
        ] + [pltpu.VMEM((1, k), F32) for k in (c1, c1, c2, c2, c3, c3)] + [
            dma(d) for d in ((kk,), (12,), (2,), (2,), (2,), (kk, 2), (5, 2), (5, 2), (5, 4), (5, 4), (5, 2), (5, hh, 2))
        ]
        feats = pl.pallas_call(
            functools.partial(_encoder_kernel, dims),
            out_shape=jax.ShapeDtypeStruct((he, we, n, c3), BF),
            in_specs=[hbm] * 13,
            out_specs=pl.BlockSpec(memory_space=pltpu.VMEM),
            scratch_shapes=scratch,
            compiler_params=pltpu.CompilerParams(collective_id=0, has_side_effects=True, vmem_limit_bytes=53 * 1024 * 1024),
        )(*[pltpu.with_memory_space_constraint(x, pltpu.HBM) for x in (img, w_down1, b_down1, w_conv1, b_conv1, w_down2, b_down2, w_conv2, b_conv2, wd3, b_down3, w_conv3, b_conv3)])
        return jnp.transpose(feats, (2, 0, 1, 3))

    tile_spec = P('batch', 'row', 'col', None)
    return jax.shard_map(local_encoder, mesh=mesh, in_specs=(tile_spec,) + (P(),) * 12, out_specs=tile_spec, check_vma=False)
```

```python
import functools

import jax
import jax.numpy as jnp
from jax import lax
from jax.experimental import pallas as pl
from jax.experimental.pallas import tpu as pltpu
from jax.sharding import PartitionSpec as P

BY_LAST = (((1,), (1,)), ((), ()))
BF = jnp.bfloat16
F32 = jnp.float32
LANES = 128
TILE = 2 * LANES
PITCH = 129


def _encoder_kernel(dims, img, wd1, bd1, wc1, bc1, wd2, bd2, wc2, bc2, wd3, bd3, wc3, bc3, out,
                    raw, xt, y1, z1, y2, z2, y3, st0, st1, st2,
                    vwd1, vwc1, vwd2, vwc2, vwd3, vwc3, wp1, wp2, wp6,
                    vb1, vb2, vb3, vb4, vb5, vb6,
                    raw_sem, w_sem, rh_send, rh_recv, xc_send, xc_recv,
                    row_send, row_recv, cor_send, cor_recv, col_send, col_recv):
    row_len, col_len = dims
    nimg = img.shape[0]
    my_row = lax.axis_index('row')
    my_col = lax.axis_index('col')
    up, down = my_row > 0, my_row < row_len - 1
    left, right = my_col > 0, my_col < col_len - 1

    def both(a, b):
        return jnp.logical_and(a, b)

    near = [(up, -1, 0), (down, 1, 0), (left, 0, -1), (right, 0, 1)]
    near += [(both(v[0], g[0]), v[1], g[2]) for v in near[:2] for g in near[2:]]

    def dev(dr, dc):
        return {'row': my_row + dr, 'col': my_col + dc}

    def raw_copy(k):
        return pltpu.make_async_copy(img.at[:, pl.ds(2 * k - 1, 2)], raw.at[k], raw_sem.at[k])

    last = raw.shape[0] - 1
    mid = last // 2
    first_copy = pltpu.make_async_copy(img.at[:, pl.ds(0, 1)], raw.at[0, :, pl.ds(1, 1)], raw_sem.at[0])
    last_copy = pltpu.make_async_copy(img.at[:, pl.ds(2 * last - 1, 1)], raw.at[last, :, pl.ds(0, 1)], raw_sem.at[last])
    def loop(count, act):
        def body(i, carry):
            act(i)
            return carry
        lax.fori_loop(0, count, body, 0)

    def middle_out(t):
        h = (t + 1) // 2
        return mid + h * (1 - 2 * (t % 2))

    weights = [(wd1, vwd1), (wc1, vwc1), (wd2, vwd2), (wc2, vwc2), (wd3, vwd3), (wc3, vwc3),
               *((x, v.at[0]) for x, v in zip((bd1, bc1, bd2, bc2, bd3, bc3), (vb1, vb2, vb3, vb4, vb5, vb6)))]
    wcopies = [pltpu.make_async_copy(s, d, w_sem.at[i]) for i, (s, d) in enumerate(weights)]
    for i in (0, 6, 1, 7):
        wcopies[i].start()
    loop(last - 1, lambda t: raw_copy(middle_out(t)).start())
    first_copy.start()
    last_copy.start()

    barrier = pltpu.get_barrier_semaphore()
    for there, dr, dc in near:
        @pl.when(there)
        def _(dr=dr, dc=dc):
            pl.semaphore_signal(barrier, inc=1, device_id=dev(dr, dc), device_id_type=pl.DeviceIdType.MESH)
    nu, nd, nl, nr = [jnp.where(x, 1, 0) for x in (up, down, left, right)]
    pl.semaphore_wait(barrier, (1 + nu + nd) * (1 + nl + nr) - 1)

    def raw_send(s):
        if s == 0:
            return pltpu.make_async_remote_copy(img.at[:, pl.ds(0, 1)], raw.at[last, :, pl.ds(1, 1)],
                                                rh_send.at[0], rh_recv.at[0], device_id=dev(-1, 0), device_id_type=pl.DeviceIdType.MESH)
        return pltpu.make_async_remote_copy(img.at[:, pl.ds(2 * last - 1, 1)], raw.at[0, :, pl.ds(0, 1)],
                                            rh_send.at[1], rh_recv.at[1], device_id=dev(1, 0), device_id_type=pl.DeviceIdType.MESH)

    for there, s in zip((up, down), range(2)):
        @pl.when(there)
        def _(s=s):
            raw_send(s).start()

    def zero(ref):
        ref[...] = jnp.zeros(ref.shape, ref.dtype)

    def wide(ref, h):
        u = ref.shape[1] - 2
        return dict(ref=ref, h=h, hl=(0, 1), first=(1, 0), last=(u, 1), hr=(u + 1, 0), real=pl.ds(1, u))

    def flat(ref, h):
        w = ref.shape[1] - 2
        return dict(ref=ref, h=h, hl=(0,), first=(1,), last=(w,), hr=(w + 1,), real=pl.ds(1, w))

    bufs = [wide(y1, y1.shape[0] - 2), wide(z1, z1.shape[0] - 2), flat(y2, y2.shape[0] - 2), wide(z2, z2.shape[0] - 2),
            flat(y3, y3.shape[0] - 2)]

    for b in bufs:
        ref, h = b['ref'], b['h']

        @pl.when(jnp.logical_not(up))
        def _(ref=ref):
            zero(ref.at[0])

        @pl.when(jnp.logical_not(down))
        def _(ref=ref, h=h):
            zero(ref.at[h + 1])

        @pl.when(jnp.logical_not(left))
        def _(ref=ref, b=b, h=h):
            for r in range(h + 2):
                zero(ref.at[(r,) + b['hl']])

        @pl.when(jnp.logical_not(right))
        def _(ref=ref, b=b, h=h):
            for r in range(h + 2):
                zero(ref.at[(r,) + b['hr']])

    @pl.when(jnp.logical_not(up))
    def _():
        for n in range(nimg):
            zero(raw.at[0, n, 0])

    @pl.when(jnp.logical_not(down))
    def _():
        for n in range(nimg):
            zero(raw.at[last, n, 1])

    xu = xt.shape[1] - 2

    @pl.when(jnp.logical_not(left))
    def _():
        for k in range(last + 1):
            zero(xt.at[k, 0, 3])

    @pl.when(jnp.logical_not(right))
    def _():
        for k in range(last + 1):
            zero(xt.at[k, xu + 1, 0])

    def row_copy(i, s):
        b = bufs[i]
        ref, h = b['ref'], b['h']
        src, dst, dr = (1, h + 1, -1) if s == 0 else (h, 0, 1)
        return pltpu.make_async_remote_copy(ref.at[src, b['real']], ref.at[dst, b['real']], row_send.at[i, s], row_recv.at[i, s],
                                            device_id=dev(dr, 0), device_id_type=pl.DeviceIdType.MESH)

    def corner_copy(i, s):
        b = bufs[i]
        ref, h = b['ref'], b['h']
        dr, dc = near[4 + s][1:]
        src = (1 if dr < 0 else h,) + (b['first'] if dc < 0 else b['last'])
        dst = (h + 1 if dr < 0 else 0,) + (b['hr'] if dc < 0 else b['hl'])
        return pltpu.make_async_remote_copy(ref.at[src], ref.at[dst], cor_send.at[i, s], cor_recv.at[i, s],
                                            device_id=dev(dr, dc), device_id_type=pl.DeviceIdType.MESH)

    def col_copy(i, r, s):
        b = bufs[i]
        ref = b['ref']
        src, dst, dc = (b['first'], b['hr'], -1) if s == 0 else (b['last'], b['hl'], 1)
        return pltpu.make_async_remote_copy(ref.at[(r + 1,) + src], ref.at[(r + 1,) + dst], col_send.at[i, s], col_recv.at[i, r, s],
                                            device_id=dev(0, dc), device_id_type=pl.DeviceIdType.MESH)

    sides = ((left, 0), (right, 1))
    from_sides = ((right, 0), (left, 1))

    def each(cases, act):
        for there, s in cases:
            @pl.when(there)
            def _(s=s):
                act(s)

    ends = list(zip((up, down), range(2)))
    from_ends = list(zip((down, up), range(2)))
    corners = [(x[0], s) for s, x in enumerate(near[4:])]
    from_corners = [(x[0], s) for s, x in enumerate(near[:3:-1])]

    def send_rows(i):
        each(ends, lambda s: row_copy(i, s).start())
        each(corners, lambda s: corner_copy(i, s).start())

    def wait_rows(i):
        each(from_ends, lambda s: row_copy(i, s).wait_recv())
        each(from_corners, lambda s: corner_copy(i, s).wait_recv())

    def xcol_copy(k, s):
        src, dst, dc = ((1, 0), (xu + 1, 0), -1) if s == 0 else ((xu, 3), (0, 3), 1)
        return pltpu.make_async_remote_copy(xt.at[(k,) + src], xt.at[(k,) + dst], xc_send.at[s], xc_recv.at[k, s],
                                            device_id=dev(0, dc), device_id_type=pl.DeviceIdType.MESH)

    def send_xcols(ks):
        each(sides, lambda s: [xcol_copy(k, s).start() for k in ks])

    def wait_xcols(*ks):
        each(from_sides, lambda s: [xcol_copy(k, s).wait_recv() for k in ks])

    for i in (0, 1, 6, 7):
        wcopies[i].wait()

    def zero_block(ref):
        def act(i):
            zero(ref.at[i])
        return act

    def fill1(i):
        dk, dc, cpar, rpar = i // 8, i // 4 % 2, i // 2 % 2, i % 2
        for j in range(2):
            wp1[(dk * 3 + dc + j) * 4 + cpar * 2 + rpar, :, pl.ds(j * LANES, LANES)] = vwd1[2 * dk + rpar, 2 * dc + cpar]

    def fill2(i):
        for j in range(2):
            wp2[i // 3 * 4 + i % 3 + j, :, pl.ds(j * LANES, LANES)] = vwc1[i // 3, i % 3]

    loop(wp1.shape[0], zero_block(wp1))
    loop(wp2.shape[0], zero_block(wp2))
    loop(16, fill1)
    loop(9, fill2)

    eye = (lax.broadcasted_iota(jnp.int32, (LANES, LANES), 0) == lax.broadcasted_iota(jnp.int32, (LANES, LANES), 1)).astype(F32).astype(BF)

    def transpose_in(k, st):
        for s in range(nimg // 2):
            rhs = raw[k, pl.ds(2 * s, 2)].reshape(TILE, LANES)
            t = lax.dot_general(eye, rhs, BY_LAST, preferred_element_type=F32)
            st[pl.ds(2 * s * PITCH, LANES), :] = t[:, :LANES]
            st[pl.ds((2 * s + 1) * PITCH, LANES), :] = t[:, LANES:]

    def transpose_out(k, st):
        for c in range(4 * xu):
            xt[k, 1 + c // 4, c % 4] = st[pl.ds(c, nimg, stride=PITCH), :].astype(BF)

    inner = (last - 1) // 3

    def take_three(it, carry):
        edge = it // inner
        ks = [edge * (last * min(d, 1)) + (1 - edge) * middle_out(3 * it + d) for d in range(3)]

        @pl.when(it < inner)
        def _():
            for k in ks:
                raw_copy(k).wait()

        @pl.when(it == inner)
        def _():
            first_copy.wait()
            last_copy.wait()
            each(from_ends, lambda s: raw_send(s).wait_recv())
        for k, st in zip(ks, (st0, st1, st2)):
            transpose_in(k, st)
        for k, st in zip(ks, (st0, st1, st2)):
            transpose_out(k, st)
        send_xcols(ks[:2])

        @pl.when(it < inner)
        def _():
            send_xcols(ks[2:])
        return carry

    def finish(acc, bias):
        return jnp.maximum(acc + bias, 0.0).astype(BF)

    def put_pairs(ref, i, v):
        for j in range(2):
            ref[i + 1, pl.ds(1, pairs), j] = v[:, j * LANES:(j + 1) * LANES].reshape(pairs, nimg, LANES)

    def rows_of(ref, idx, w):
        v = ref[idx]
        return v.reshape(w * nimg, v.shape[-1])

    def wait_pair(i, a, h):
        each(from_sides, lambda s: [col_copy(i, r, s).wait_recv() for r in (a, h - 1 - a)])

    def step_of(t, n, p):
        up_now = (t + n - p) // n
        return (1 - up_now) * (n - 1 - t) + up_now * (t - p)

    def wait_conv(i, t, a, h, p):
        n = h // 2
        seen = n - 1 - p if p else n

        if p:
            @pl.when(t == 0)
            def _():
                wait_pair(i, n - 1, h)

            @pl.when(t < p)
            def _():
                wait_pair(i, a - 1, h)

        @pl.when(t == p)
        def _():
            wait_pair(i, 0, h)
            wait_rows(i)

        @pl.when(jnp.logical_and(t >= p, a + 1 < seen))
        def _():
            wait_pair(i, a + 1, h)

    def wait_down(i, a, h):
        @pl.when(a == 0)
        def _():
            wait_pair(i, 0, 2 * h)
            wait_rows(i)
        wait_pair(i, 2 * a + 1, 2 * h)

        @pl.when(a < h // 2 - 1)
        def _():
            wait_pair(i, 2 * a + 2, 2 * h)

    def send(i, t, a, h, e):
        @pl.when(t == e)
        def _():
            send_rows(i)
        each(sides, lambda s: [col_copy(i, r, s).start() for r in (a, h - 1 - a)])

    pairs = y1.shape[1] - 2
    bias1 = jnp.concatenate([vb1[...], vb1[...]], axis=-1)
    h1 = y1.shape[0] - 2

    e1 = 3

    def down1(t, carry):
        a = step_of(t, h1 // 2, e1)

        @pl.when(t == 0)
        def _():
            wait_xcols(mid)

        @pl.when(t < e1)
        def _():
            wait_xcols(a, last - a)

        @pl.when(t == e1)
        def _():
            wait_xcols(0, last)

        @pl.when(jnp.logical_and(t >= e1, a + 1 < h1 // 2 - e1))
        def _():
            wait_xcols(a + 1, last - 1 - a)
        for i in (a, h1 - 1 - a):
            parts = []
            for dk in range(2):
                for p in range(3, 9):
                    parts.append(rows_of(xt, (i + dk, pl.ds(p // 4, pairs), p % 4), pairs))
            acc = jnp.dot(jnp.concatenate(parts, axis=-1), wp1[...].reshape(6 * TILE, TILE), preferred_element_type=F32)
            v = finish(acc, bias1)
            put_pairs(y1, i, v)
        send(0, t, a, h1, e1)
        return carry

    def phase(ph, carry):
        lax.fori_loop(inner * ph, inner + ph, take_three, 0)

        @pl.when(ph == 0)
        def _():
            for i in range(2, 6):
                wcopies[i].start()
                wcopies[i + 6].start()
        lax.fori_loop((e1 - 2) * ph, e1 - 2 + (h1 // 2 - e1 + 2) * ph, down1, 0)
        return carry

    lax.fori_loop(0, 2, phase, 0)

    bias2 = jnp.concatenate([vb2[...], vb2[...]], axis=-1)

    def conv1(t, carry):
        a = step_of(t, h1 // 2, 1)
        wait_conv(0, t, a, h1, 1)
        for i in (a, h1 - 1 - a):
            parts = []
            for p in range(3):
                for s in range(1, 5):
                    parts.append(rows_of(y1, (i + p, pl.ds(s // 2, pairs), s % 2), pairs))
            acc = jnp.dot(jnp.concatenate(parts, axis=-1), wp2[...].reshape(6 * TILE, TILE), preferred_element_type=F32)
            v = finish(acc, bias2)
            put_pairs(z1, i, v)
        send(1, t, a, h1, 1)
        return carry

    lax.fori_loop(0, h1 // 2, conv1, 0)

    ch3 = out.shape[-1]
    h2 = y2.shape[0] - 2
    w2 = y2.shape[1] - 2
    for i in (2, 8):
        wcopies[i].wait()

    def down2(t, carry):
        a = t
        wait_down(1, a, h2)
        for i in (a, h2 - 1 - a):
            parts = []
            for p in range(4):
                for s in range(1, 5):
                    parts.append(rows_of(z1, (2 * i + p, pl.ds(s // 2, w2), s % 2), w2))
            acc = jnp.dot(jnp.concatenate(parts, axis=-1), vwd2[...].reshape(16 * LANES, TILE), preferred_element_type=F32)
            y2[i + 1, pl.ds(1, w2)] = finish(acc, vb3[...]).reshape(w2, nimg, TILE)
        send(2, t, a, h2, 0)
        return carry

    lax.fori_loop(0, h2 // 2, down2, 0)
    for i in (3, 9, 5):
        wcopies[i].wait()

    def fill6(i):
        wp6[i, pl.ds(0, ch3), :] = vwc3[i // 3, i % 3]
        wp6[i, pl.ds(ch3, wp6.shape[1] - ch3), :] = jnp.zeros((wp6.shape[1] - ch3, ch3), BF)

    loop(9, fill6)

    def conv2(t, carry):
        a = t
        wait_conv(2, t, a, h2, 0)
        for i in (a, h2 - 1 - a):
            parts = []
            for p in range(3):
                for q in range(3):
                    parts.append(rows_of(y2, (i + p, pl.ds(q, w2)), w2))
            acc = jnp.dot(jnp.concatenate(parts, axis=-1), vwc2[...].reshape(9 * TILE, TILE), preferred_element_type=F32)
            v = finish(acc, vb4[...]).reshape(w2 // 2, 2, nimg, TILE)
            z2[i + 1, pl.ds(1, w2 // 2), 0] = v[:, 0]
            z2[i + 1, pl.ds(1, w2 // 2), 1] = v[:, 1]
        send(3, t, a, h2, 0)
        return carry

    lax.fori_loop(0, h2 // 2, conv2, 0)

    h3 = y3.shape[0] - 2
    w3 = y3.shape[1] - 2
    for i in (4, 10, 11):
        wcopies[i].wait()

    def down3(t, carry):
        a = t
        wait_down(3, a, h3)
        ii = (a, h3 - 1 - a)
        parts, wts = [], []
        for p in range(4):
            for s in range(1, 5):
                parts.append(jnp.concatenate([rows_of(z2, (2 * i + p, pl.ds(s // 2, w3), s % 2), w3) for i in ii], axis=0))
                wts.append(vwd3[p, s - 1])
        acc = lax.dot_general(jnp.concatenate(parts, axis=-1), jnp.concatenate(wts, axis=-1), BY_LAST, preferred_element_type=F32)
        v = finish(acc, vb5[...])
        v = jnp.concatenate([v, jnp.zeros((v.shape[0], y3.shape[-1] - ch3), BF)], axis=-1)
        for n, i in enumerate(ii):
            y3[i + 1, pl.ds(1, w3)] = v[n * w3 * nimg:(n + 1) * w3 * nimg].reshape(w3, nimg, y3.shape[-1])
        send(4, t, a, h3, 0)
        return carry

    lax.fori_loop(0, h3 // 2, down3, 0)

    def conv3(t, carry):
        @pl.when(t == 1)
        def _():
            for r in range(h3 // 2):
                wait_pair(4, r, h3)
            wait_rows(4)
        top, bottom, lo, hi = 1 - t, h3 - 2 + t, 1 - t, w3 - 2 + t
        strips = [(i, 1, w3 - 2) for i in (top, bottom)] + [(i, c, 1) for i in (top, bottom, *range(1, h3 - 1)) for c in (lo, hi)]
        parts = []
        for p in range(3):
            for q in range(3):
                parts.append(jnp.concatenate([rows_of(y3, (i + p, pl.ds(c + q, w)), w) for i, c, w in strips], axis=0))
        acc = jnp.dot(jnp.concatenate(parts, axis=-1), wp6[...].reshape(9 * wp6.shape[1], ch3), preferred_element_type=F32)
        v = finish(acc, vb6[...])
        at = 0
        for i, c, w in strips:
            out[i, pl.ds(c, w)] = v[at:at + w * nimg].reshape(w, nimg, ch3)
            at += w * nimg
        return carry

    lax.fori_loop(0, 2, conv3, 0)

    each(ends, lambda s: raw_send(s).wait_send())

    def drain_cols(ref, rows, at, sem):
        whole = ref.at[(rows,) + at]
        pltpu.make_async_remote_copy(whole, whole, sem, sem, device_id=dev(0, 0), device_id_type=pl.DeviceIdType.MESH).wait_send()

    each(sides, lambda s: drain_cols(xt, pl.ds(0, last + 1), (1, 0), xc_send.at[s]))
    for i, b in enumerate(bufs):
        each(ends, lambda s: row_copy(i, s).wait_send())
        each(corners, lambda s: corner_copy(i, s).wait_send())
        each(sides, lambda s: drain_cols(b['ref'], pl.ds(1, b['h']), b['first'], col_send.at[i, s]))


def solution(mesh):
    dims = (mesh.shape['row'], mesh.shape['col'])

    def local_encoder(images, w_down1, b_down1, w_conv1, b_conv1, w_down2, b_down2, w_conv2, b_conv2, w_down3, b_down3, w_conv3, b_conv3):
        n, h, w, c = images.shape
        img = jnp.transpose(images, (0, 1, 3, 2))
        wd3 = jnp.transpose(w_down3, (0, 1, 3, 2))
        c1, c2, c3 = w_conv1.shape[-1], w_conv2.shape[-1], w_conv3.shape[-1]
        c3p = pl.cdiv(c3, LANES) * LANES
        hbm = pl.BlockSpec(memory_space=pl.ANY)
        dma = pltpu.SemaphoreType.DMA
        hh, hq, he = h // 2, h // 4, h // 8
        wq, we = w // 4, w // 8
        kk = hh + 1
        scratch = [
            pltpu.VMEM((kk, n, 2, c, w), BF),
            pltpu.VMEM((kk, wq + 2, 4, n, 2 * c), BF),
            pltpu.VMEM((hh + 2, wq + 2, 2, n, c1), BF),
            pltpu.VMEM((hh + 2, wq + 2, 2, n, c1), BF),
            pltpu.VMEM((hq + 2, wq + 2, n, c2), BF),
            pltpu.VMEM((hq + 2, we + 2, 2, n, c2), BF),
            pltpu.VMEM((he + 2, we + 2, n, c3p), BF),
        ] + [pltpu.VMEM((n * PITCH, LANES), F32)] * 3 + [
            pltpu.VMEM(x.shape, BF) for x in (w_down1, w_conv1, w_down2, w_conv2, wd3, w_conv3)
        ] + [
            pltpu.VMEM((24, c, TILE), BF),
            pltpu.VMEM((12, c1, TILE), BF),
            pltpu.VMEM((9, c3p, c3), BF),
        ] + [pltpu.VMEM((1, k), F32) for k in (c1, c1, c2, c2, c3, c3)] + [
            dma(d) for d in ((kk,), (12,), (2,), (2,), (2,), (kk, 2), (5, 2), (5, 2), (5, 4), (5, 4), (5, 2), (5, hh, 2))
        ]
        feats = pl.pallas_call(
            functools.partial(_encoder_kernel, dims),
            out_shape=jax.ShapeDtypeStruct((he, we, n, c3), BF),
            in_specs=[hbm] * 13,
            out_specs=pl.BlockSpec(memory_space=pltpu.VMEM),
            scratch_shapes=scratch,
            compiler_params=pltpu.CompilerParams(collective_id=0, has_side_effects=True, vmem_limit_bytes=53 * 1024 * 1024),
        )(*[pltpu.with_memory_space_constraint(x, pltpu.HBM) for x in (img, w_down1, b_down1, w_conv1, b_conv1, w_down2, b_down2, w_conv2, b_conv2, wd3, b_down3, w_conv3, b_conv3)])
        return jnp.transpose(feats, (2, 0, 1, 3))

    tile_spec = P('batch', 'row', 'col', None)
    return jax.shard_map(local_encoder, mesh=mesh, in_specs=(tile_spec,) + (P(),) * 12, out_specs=tile_spec, check_vma=False)
```
